32 devices in a mesh: zero: 8 (over z, x), model: 4 (over y, core).
Axes of the slice: x: 2, y: 2, z: 4, core: 2. Of those that a mesh axis runs over, the one named last changes fastest.
Arguments:
- w_query: bfloat16 [4096, 4096], P('zero', 'model'), may hold values from -0.125 to 0.125
- low_query: bfloat16 [4096, 16], P('zero'), may hold values from -0.09375 to 0.09375
- high_query: bfloat16 [16, 4096], P(None, 'model'), may hold values from -1.5 to 1.5
- w_key: bfloat16 [4096, 4096], P('zero', 'model'), may hold values from -0.125 to 0.125
- low_key: bfloat16 [4096, 16], P('zero'), may hold values from -0.09375 to 0.09375
- high_key: bfloat16 [16, 4096], P(None, 'model'), may hold values from -1.5 to 1.5
- w_value: bfloat16 [4096, 4096], P('zero', 'model'), may hold values from -0.125 to 0.125
- low_value: bfloat16 [4096, 16], P('zero'), may hold values from -0.09375 to 0.09375
- high_value: bfloat16 [16, 4096], P(None, 'model'), may hold values from -1.5 to 1.5
- norm_train: float32 [4096], P(('zero', 'model')), may hold values from 0.25 to 1.75
- norm_step: float32 [4096], P(('zero', 'model')), may hold values from -0.3 to 0.3
Outputs:
- serving_query: bfloat16 [4096, 4096], P(None, 'model')
- serving_key: bfloat16 [4096, 4096], P(None, 'model')
- serving_value: bfloat16 [4096, 4096], P(None, 'model')
- factor_query: float32 [4096], P('model')
- factor_key: float32 [4096], P('model')
- factor_value: float32 [4096], P('model')
- serve_norm: bfloat16 [4096], replicated
The draws below stay inside these ranges and needn't reach their ends.
All inputs are finite; a program needn't handle non-finite values. Where the reference program divides by a largest or mean magnitude, that divisor is 1e-20 or more.
Results may differ from the reference program's by a relative error of at most 0.001.
Values may be sent and summed in bfloat16 or wider, within the bound.
A program may use at most 128 MiB of HBM per device.

```python
import jax
import jax.numpy as jnp

D_MODEL = 4096
Q_DIM = 4096
KV_DIM = 4096
RANK = 16


def spiked(array, stream_key, source, target, parts, factor):
    def block_of(axis_at):
        return (jnp.arange(array.shape[axis_at]) // (array.shape[axis_at] // parts)).reshape((-1,) + (1,) * (array.ndim - 1 - axis_at))

    first = jax.random.permutation(stream_key, parts)[block_of(target)]
    other_side = (block_of(target) + parts // 2) % parts
    return jnp.where((block_of(source) == first) | (block_of(source) == other_side), factor * array, array)


def block_levels(key, dims, cuts, least, largest):
    loudness = 1.0
    for axis_at, parts in cuts:
        heights = jax.random.uniform(jax.random.fold_in(jax.random.fold_in(key, 6), axis_at), (parts,), jnp.float32, least / len(cuts), largest / len(cuts))
        loudness = loudness * jnp.repeat(jnp.exp(heights), dims[axis_at] // parts).reshape((-1,) + (1,) * (len(dims) - 1 - axis_at))
    return loudness


def noise(own_key, extent, width, bound, cuts=(), kind=jnp.bfloat16):
    array = width * jax.random.normal(own_key, extent, jnp.float32)
    if cuts:
        array = array * block_levels(own_key, extent, cuts, -0.22, 0.18)
    return jnp.clip(array, -bound, bound).astype(kind)


def bell_draw_with(rng, extent, scale, reach, pieces, heavy, held_as=jnp.bfloat16):
    drawn = scale * jax.random.normal(rng, extent, jnp.float32)
    if pieces:
        drawn = drawn * block_levels(rng, extent, pieces, -0.22, 0.18)
    return jnp.clip(spiked(drawn, jax.random.fold_in(rng, 3), *heavy), -reach, reach).astype(held_as)


def setup_inputs(seed: int = 0) -> dict:
    key_list = jax.random.split(jax.random.key(seed), 12)
    return {
        "w_query": bell_draw_with(key_list[0], (D_MODEL, Q_DIM), D_MODEL ** -0.5, 0.125, ((0, 8), (1, 4)), (0, 1, 8, 2.0)),
        "low_query": noise(key_list[1], (D_MODEL, RANK), D_MODEL ** -0.5, 0.09375, ((0, 8),)),
        "high_query": noise(key_list[2], (RANK, Q_DIM), RANK ** -0.5, 1.5, ((1, 4),)),
        "w_key": bell_draw_with(key_list[3], (D_MODEL, KV_DIM), D_MODEL ** -0.5, 0.125, ((0, 8), (1, 4)), (0, 1, 8, 2.0)),
        "low_key": noise(key_list[4], (D_MODEL, RANK), D_MODEL ** -0.5, 0.09375, ((0, 8),)),
        "high_key": noise(key_list[5], (RANK, KV_DIM), RANK ** -0.5, 1.5, ((1, 4),)),
        "w_value": bell_draw_with(key_list[6], (D_MODEL, KV_DIM), D_MODEL ** -0.5, 0.125, ((0, 8), (1, 4)), (0, 1, 8, 2.0)),
        "low_value": noise(key_list[7], (D_MODEL, RANK), D_MODEL ** -0.5, 0.09375, ((0, 8),)),
        "high_value": noise(key_list[8], (RANK, KV_DIM), RANK ** -0.5, 1.5, ((1, 4),)),
        "norm_train": jnp.clip(1.0 + 0.15 * jax.random.normal(key_list[9], (D_MODEL,), jnp.float32), 0.25, 1.75),
        "norm_step": jnp.clip(jax.random.uniform(key_list[10], (D_MODEL,), jnp.float32, -0.3, 0.3) * block_levels(key_list[10], (D_MODEL,), ((0, 32),), -0.4, 0.0), -0.3, 0.3),
    }


mix_rate = 0.5


def reference(w_query, low_query, high_query, w_key, low_key, high_key, w_value, low_value, high_value, norm_train, norm_step):
    whole_query = w_query.astype(jnp.float32) + mix_rate * jnp.dot(low_query, high_query, preferred_element_type=jnp.float32)
    whole_key = w_key.astype(jnp.float32) + mix_rate * jnp.dot(low_key, high_key, preferred_element_type=jnp.float32)
    whole_value = w_value.astype(jnp.float32) + mix_rate * jnp.dot(low_value, high_value, preferred_element_type=jnp.float32)
    factor_query = jnp.sum(jnp.abs(whole_query), axis=0) / D_MODEL
    serving_query = (whole_query / factor_query).astype(jnp.bfloat16)
    factor_key = jnp.sum(jnp.abs(whole_key), axis=0) / D_MODEL
    serving_key = (whole_key / factor_key).astype(jnp.bfloat16)
    factor_value = jnp.sum(jnp.abs(whole_value), axis=0) / D_MODEL
    serving_value = (whole_value / factor_value).astype(jnp.bfloat16)
    serve_norm = (norm_train + norm_step).astype(jnp.bfloat16)
    return serving_query, serving_key, serving_value, factor_query, factor_key, factor_value, serve_norm
```

```python
import functools

import jax
import jax.numpy as jnp
from jax import lax
from jax.experimental import pallas as pl
from jax.experimental.pallas import tpu as pltpu
from jax.sharding import PartitionSpec as P

MESH = pl.DeviceIdType.MESH
mix_rate = 0.5
VMEM_MOST = 67_043_328
SPARE = 65_536
COLUMNS = 2
PIECES = 6
RAW = 2
LOW, NORM = PIECES, PIECES + 1
WRITES = 4
FIRST = 1


def queues_of(z, length):
    every = [LOW] + list(range(PIECES)) + [NORM]
    late = list(range(PIECES // 2, PIECES))
    early = [c for c in every if c not in late]
    out = {"up": [], "down": [], "side": []}
    if z < length - 1:
        out["up"] += [(z - s, 0, c) for s in range(z + 1) for c in every]
        if z == 0:
            out["up"] += [(0, 1, c) for c in every]
        if z == length - 2:
            out["up"] += [(z, 1, c) for c in late]
    if z > 0:
        out["down"] += [(z + s, 0, c) for s in range(length - z) for c in every]
        if z == length - 1:
            out["down"] += [(z, 1, c) for c in every]
        if z == 1:
            out["down"] += [(z, 1, c) for c in late]
    for b in sorted(range(length), key=lambda b: (abs(b - z), b)):
        pieces = every
        if (z, b) in ((0, 1), (length - 1, length - 2)):
            pieces = early
        if (z, b) in ((1, 0), (length - 2, length - 1)):
            pieces = []
        out["side"] += [(b, 0, c) for c in pieces]
    return out


def order_of(length):
    size = [1.0] * PIECES + [0.04, 0.01]
    queues = [queues_of(z, length) for z in range(length)]
    far = 1e9
    there = [{} for _ in range(length)]
    for z in range(length):
        for c in range(len(size)):
            there[z][z, 0, c] = 0.0
    for _ in range(4 * length):
        for z in range(length):
            for name, queue in queues[z].items():
                now = 0.0
                for b, o, c in queue:
                    now = max(now, there[z].get((b, o, c), far)) + size[c]
                    to = {"up": z + 1, "down": z - 1, "side": z}[name]
                    key = (b, 1 - o if name == "side" else o, c)
                    there[to][key] = now
    result = []
    for z in range(length):
        events = []
        for name, queue in queues[z].items():
            key = 0.0
            for at, (b, o, c) in enumerate(queue):
                key = max(key, there[z][b, o, c])
                events.append((key, at, name, b, o, c))
        assert max(e[0] for e in events) < far
        result.append((sorted(events), there[z]))
    return result


def gather_kernel(
    n_zero, n_model,
    w_q, w_k, w_v, l_q, l_k, l_v, h_q, h_k, h_v, n_a, n_b,
    s_q, s_k, s_v, factors, norms,
    w_vm, h_vm, l_vm, lows, raws, sums, scales, na_vm, nb_vm,
    send_sem, recv_sem, load_sem, ssend_sem, srecv_sem, nsend_sem, nrecv_sem, ready_sem,
):
    w, low, high = (w_q, w_k, w_v), (l_q, l_k, l_v), (h_q, h_k, h_v)
    served = (s_q, s_k, s_v)
    length = n_zero // COLUMNS
    zero, model = lax.axis_index("zero"), lax.axis_index("model")
    place, column = zero // COLUMNS, zero % COLUMNS
    rows, width = w_q.shape
    rank = l_q.shape[0]
    half = rows // 2
    me = zero * n_model + model
    orders = order_of(length)

    barrier = pltpu.get_barrier_semaphore()
    partners = [(zero, lax.rem(model + k, n_model)) for k in range(1, n_model)]
    partners.append((place * COLUMNS + 1 - column, model))
    for to in partners:
        pl.semaphore_signal(barrier, inc=1, device_id=to, device_id_type=MESH)

    @pl.when(place > 0)
    def _():
        pl.semaphore_signal(barrier, inc=1, device_id=(zero - COLUMNS, model), device_id_type=MESH)

    @pl.when(place < length - 1)
    def _():
        pl.semaphore_signal(barrier, inc=1, device_id=(zero + COLUMNS, model), device_id_type=MESH)

    loads = []
    for m in range(3):
        into = lows.at[zero] if m == 0 else l_vm.at[m - 1]
        loads.append(pltpu.make_async_copy(low[m], into, load_sem.at[m]))
    for m in range(3):
        loads.append(pltpu.make_async_copy(w[m], w_vm.at[m], load_sem.at[3 + m]))
        loads.append(pltpu.make_async_copy(high[m], h_vm.at[m], load_sem.at[6 + m]))
    loads.append(pltpu.make_async_copy(n_a, na_vm, load_sem.at[9]))
    loads.append(pltpu.make_async_copy(n_b, nb_vm, load_sem.at[10]))
    for load in loads:
        load.start()

    def block_at(b, o):
        return b * COLUMNS + (column if o == 0 else 1 - column)

    def part(ref, block, c):
        first = pl.multiple_of(block * rows, rows) + (c % 2) * half
        return ref.at[pl.ds(pl.multiple_of(first, half), half)]

    def landing(block, c):
        if c == LOW:
            return lows.at[block]
        if c == NORM:
            return norms.at[pl.ds(block * n_model, n_model)]
        return part(raws if c < RAW else served[c // 2], block, c)

    lane_of = {"up": 0, "down": 1, "side": 2}

    def copy_of(z, name, at, b, o, c):
        block = block_at(b, o)
        target = {
            "up": (z + 1) * COLUMNS + column,
            "down": (z - 1) * COLUMNS + column,
            "side": z * COLUMNS + 1 - column,
        }[name]
        source = landing(block, c)
        if b == z and o == 0:
            if c < RAW:
                source = w_q.at[pl.ds((c % 2) * half, half)]
            if c == LOW:
                source = l_q
        return pltpu.make_async_remote_copy(
            src_ref=source,
            dst_ref=landing(block, c),
            send_sem=send_sem.at[lane_of[name], at],
            recv_sem=recv_sem.at[block, c],
            device_id=(target, model),
            device_id_type=MESH,
        )

    def arrive(b, o, c):
        block = block_at(b, o)
        pltpu.make_async_copy(
            landing(block, c), landing(block, c), recv_sem.at[block, c]
        ).wait()

    def send_own(z, pieces):
        for key, at, name, b, o, c in orders[z][0]:
            if b == z and o == 0 and c in pieces:
                copy_of(z, name, at, b, o, c).start()

    def ready(z, way):
        pl.semaphore_signal(
            ready_sem.at[way], inc=1, device_id=(zero + (1 - 2 * way) * COLUMNS, model), device_id_type=MESH
        )

    for z in range(length):

        @pl.when(place == z)
        def _(z=z):
            pl.semaphore_wait(barrier, len(partners) + (z > 0) + (z < length - 1))
            send_own(z, (LOW, *range(FIRST)))
            if z > 0:
                pl.semaphore_wait(ready_sem.at[0], 1)
            if z < length - 1:
                ready(z, 0)
                pl.semaphore_wait(ready_sem.at[1], 1)
            if z > 0:
                ready(z, 1)

    for load in loads:
        load.wait()

    def whole_of(m, low_ref, source, at):
        mixed = lax.dot_general(
            low_ref[:, at], h_vm[m], (((0,), (0,)), ((), ())), preferred_element_type=jnp.float32
        )
        return source[at, :].astype(jnp.float32) + mix_rate * mixed

    def own_low(m):
        return lows.at[zero] if m == 0 else l_vm.at[m - 1]

    tile = 128
    for m in range(3):

        def add(i, total, m=m):
            at = pl.ds(pl.multiple_of(i * tile, tile), tile)
            whole = whole_of(m, own_low(m), w_vm.at[m], at)
            return total + jnp.sum(jnp.abs(whole).reshape(tile // 8, 8, width), axis=0)

        total = lax.fori_loop(0, rows // tile, add, jnp.zeros((8, width), jnp.float32))
        sums[zero, :, m * width : (m + 1) * width] = jnp.sum(total, axis=0, keepdims=True)
    norms[pl.ds(me, 1)] = (na_vm[...] + nb_vm[...])[None]

    def sum_copy(k):
        to = lax.rem(zero + k, n_zero)
        return pltpu.make_async_remote_copy(
            src_ref=sums.at[zero],
            dst_ref=sums.at[zero],
            send_sem=ssend_sem.at[k],
            recv_sem=srecv_sem.at[zero],
            device_id=(to, model),
            device_id_type=MESH,
        )

    def norm_copy(k):
        return pltpu.make_async_remote_copy(
            src_ref=norms.at[me],
            dst_ref=norms.at[me],
            send_sem=nsend_sem.at[k],
            recv_sem=nrecv_sem.at[model],
            device_id=partners[k - 1],
            device_id_type=MESH,
        )

    for k in range(1, n_zero):
        sum_copy(k).start()
    for z in range(length):

        @pl.when(place == z)
        def _(z=z):
            send_own(z, tuple(range(FIRST, RAW)))

    for k in range(1, n_model):
        norm_copy(k).start()

    for k in range(1, n_zero):
        origin = lax.rem(zero + k, n_zero)
        pltpu.make_async_copy(sums.at[origin], sums.at[origin], srecv_sem.at[origin]).wait()
    total = sums[0]
    for b in range(1, n_zero):
        total = total + sums[b]
    factor = total / (rows * n_zero)
    factors[...] = factor
    scales[...] = 1.0 / factor

    def finish(m, block, low_ref, source):
        base = pl.multiple_of(block * rows, rows)

        def step(i, carry):
            first = pl.multiple_of(i * tile, tile)
            whole = whole_of(m, low_ref, source, pl.ds(first, tile))
            to = pl.ds(pl.multiple_of(base + first, tile), tile)
            served[m][to, :] = (whole * scales[:, m * width : (m + 1) * width]).astype(s_q.dtype)
            return carry

        lax.fori_loop(0, rows // tile, step, 0)

    for m in (1, 2, 0):
        finish(m, zero, own_low(m), w_vm.at[m])
    for k in range(1, n_model):
        origin = lax.rem(model + k, n_model)
        mine = norms.at[zero * n_model + origin]
        pltpu.make_async_copy(mine, mine, nrecv_sem.at[origin]).wait()

    for z in range(length):

        @pl.when(place == z)
        def _(z=z):
            send_own(z, (*range(RAW, PIECES), NORM))
            events, there = orders[z]
            items = [(key, 0, at, name, b, o, c) for key, at, name, b, o, c in events]
            for b in range(length):
                for o in range(COLUMNS):
                    if (b, o) != (z, 0):
                        when = max(there[b, o, c] for c in (*range(RAW), LOW))
                        items.append((when, 1, 0, "", b, o, 0))
            seen = set()

            def need(b, o, c):
                if (b, o) != (z, 0) and (b, o, c) not in seen:
                    seen.add((b, o, c))
                    arrive(b, o, c)

            for _, kind, at, name, b, o, c in sorted(items):
                if kind == 0:
                    if (b, o) != (z, 0):
                        need(b, o, c)
                        copy_of(z, name, at, b, o, c).start()
                    continue
                for piece in (*range(RAW), LOW):
                    need(b, o, piece)
                block = block_at(b, o)
                raw = raws.at[pl.ds(pl.multiple_of(block * rows, rows), rows)]
                finish(0, block, lows.at[block], raw)
            for b in range(length):
                for o in range(COLUMNS):
                    for c in range(PIECES + 2):
                        need(b, o, c)
            for key, at, name, b, o, c in events:
                copy_of(z, name, at, b, o, c).wait_send()

    for k in range(1, n_zero):
        sum_copy(k).wait_send()
    for k in range(1, n_model):
        norm_copy(k).wait_send()


def write_kernel(s_q, s_k, s_v, factors, norms, o_q, o_k, o_v, f_q, f_k, f_v, norm, sem):
    rows = s_q.shape[0] // WRITES
    width = s_q.shape[1]
    copies = []
    for m, (s, o) in enumerate(((s_q, o_q), (s_k, o_k), (s_v, o_v))):
        for i in range(WRITES):
            part = pl.ds(i * rows, rows)
            copies.append(pltpu.make_async_copy(s.at[part], o.at[part], sem.at[m * WRITES + i]))
            copies[-1].start()
    for m, f in enumerate((f_q, f_k, f_v)):
        f[...] = factors[:, m * width : (m + 1) * width]
    norm[...] = norms[...].reshape(norm.shape).astype(norm.dtype)
    for copy in copies:
        copy.wait()


def on_lines(n_zero, n_model, w_q, l_q, h_q, w_k, l_k, h_k, w_v, l_v, h_v, n_a, n_b):
    rows, width = w_q.shape
    rank = l_q.shape[1]
    d_model = rows * n_zero
    count = n_zero * n_model
    share = n_a.shape[0]
    sends = (n_zero // COLUMNS) * (PIECES + 2) + PIECES
    f32, bf16 = jnp.float32, jnp.bfloat16
    shape = jax.ShapeDtypeStruct
    anywhere = pl.BlockSpec(memory_space=pl.ANY)
    inside = pl.BlockSpec(memory_space=pltpu.VMEM)
    dma = pltpu.SemaphoreType.DMA
    tall = (d_model, width)
    s_q, s_k, s_v, factors, norms = pl.pallas_call(
        functools.partial(gather_kernel, n_zero, n_model),
        out_shape=(pltpu.VMEM(tall, bf16),) * 3
        + (pltpu.VMEM((1, 3 * width), f32), pltpu.VMEM((count, 1, share), f32)),
        in_specs=[anywhere] * 11,
        out_specs=(inside,) * 5,
        scratch_shapes=[
            pltpu.VMEM((3, rows, width), bf16),
            pltpu.VMEM((3, rank, width), bf16),
            pltpu.VMEM((2, rank, rows), bf16),
            pltpu.VMEM((n_zero, rank, rows), bf16),
            pltpu.VMEM(tall, bf16),
            pltpu.VMEM((n_zero, 1, 3 * width), f32),
            pltpu.VMEM((1, 3 * width), f32),
            pltpu.VMEM((1, share), f32),
            pltpu.VMEM((1, share), f32),
            dma((3, sends)),
            dma((n_zero, PIECES + 2)),
            dma((11,)),
            dma((n_zero,)),
            dma((n_zero,)),
            dma((n_model,)),
            dma((n_model,)),
            pltpu.SemaphoreType.REGULAR((2,)),
        ],
        compiler_params=pltpu.CompilerParams(
            collective_id=0, has_side_effects=True, vmem_limit_bytes=VMEM_MOST - 3 * d_model * width * 2 - SPARE
        ),
    )(w_q, w_k, w_v, l_q.T, l_k.T, l_v.T, h_q, h_k, h_v, n_a.reshape(1, share), n_b.reshape(1, share))
    *served, f_q, f_k, f_v, norm = pl.pallas_call(
        write_kernel,
        out_shape=(shape(tall, bf16),) * 3 + (shape((1, width), f32),) * 3 + (shape((count, share), bf16),),
        in_specs=[anywhere] * 3 + [inside] * 2,
        out_specs=(anywhere,) * 3 + (inside,) * 4,
        scratch_shapes=[dma((3 * WRITES,))],
        compiler_params=pltpu.CompilerParams(
            vmem_limit_bytes=4 * 1024 * 1024
        ),
    )(s_q, s_k, s_v, factors, norms)
    return (*served, f_q.reshape(width), f_k.reshape(width), f_v.reshape(width), norm.reshape(count * share))


def plain(n_zero, n_model, w_q, l_q, h_q, w_k, l_k, h_k, w_v, l_v, h_v, n_a, n_b):
    d_model = w_q.shape[0] * n_zero
    wholes = [
        w.astype(jnp.float32) + mix_rate * jnp.dot(l, h, preferred_element_type=jnp.float32)
        for w, l, h in ((w_q, l_q, h_q), (w_k, l_k, h_k), (w_v, l_v, h_v))
    ]
    totals = lax.psum([jnp.sum(jnp.abs(whole), axis=0) for whole in wholes], "zero")
    factors = [total / d_model for total in totals]
    serving = [
        lax.all_gather((whole / factor).astype(jnp.bfloat16), "zero", axis=0, tiled=True)
        for whole, factor in zip(wholes, factors)
    ]
    norm = lax.all_gather(
        (n_a + n_b).astype(jnp.bfloat16), ("zero", "model"), axis=0, tiled=True
    )
    return (*serving, *factors, norm)


def solution(mesh):
    n_zero, n_model = mesh.shape["zero"], mesh.shape["model"]
    lines = n_zero == 2 * n_model
    tall, low, wide = P("zero", "model"), P("zero", None), P(None, "model")
    return jax.shard_map(
        functools.partial(on_lines if lines else plain, n_zero, n_model),
        mesh=mesh,
        in_specs=(tall, low, wide) * 3 + (P(("zero", "model")),) * 2,
        out_specs=(wide,) * 3 + (P("model"),) * 3 + (P(),),
        check_vma=False,
    )
```

```python
import functools

import jax
import jax.numpy as jnp
from jax import lax
from jax.experimental import pallas as pl
from jax.experimental.pallas import tpu as pltpu
from jax.sharding import PartitionSpec as P

MESH = pl.DeviceIdType.MESH
mix_rate = 0.5
VMEM_MOST = 67_043_328
SPARE = 65_536
COLUMNS = 2
PARTS = ((0, 0, 1), (0, 1, 1), (0, 2, 2), (1, 0, 2), (1, 2, 2), (2, 0, 2), (2, 2, 2))
PIECES = len(PARTS)
RAW = 2
LATE = (4, 5, 6)
LOW, NORM = PIECES, PIECES + 1
WRITES = 4
FIRST = 1


def queues_of(z, length):
    every = [LOW] + list(range(PIECES)) + [NORM]
    late = list(LATE)
    early = [c for c in every if c not in late]
    out = {"up": [], "down": [], "side": []}
    if z < length - 1:
        out["up"] += [(z - s, 0, c) for s in range(z + 1) for c in every]
        if z == 0:
            out["up"] += [(0, 1, c) for c in every]
        if z == length - 2:
            out["up"] += [(z, 1, c) for c in late]
    if z > 0:
        out["down"] += [(z + s, 0, c) for s in range(length - z) for c in every]
        if z == length - 1:
            out["down"] += [(z, 1, c) for c in every]
        if z == 1:
            out["down"] += [(z, 1, c) for c in late]
    for b in sorted(range(length), key=lambda b: (abs(b - z), b)):
        pieces = every
        if (z, b) in ((0, 1), (length - 1, length - 2)):
            pieces = early
        if (z, b) in ((1, 0), (length - 2, length - 1)):
            pieces = []
        out["side"] += [(b, 0, c) for c in pieces]
    return out


def order_of(length):
    size = [part[2] / 2 for part in PARTS] + [0.02, 0.01]
    queues = [queues_of(z, length) for z in range(length)]
    far = 1e9
    there = [{} for _ in range(length)]
    for z in range(length):
        for c in range(len(size)):
            there[z][z, 0, c] = 0.0
    for _ in range(4 * length):
        for z in range(length):
            for name, queue in queues[z].items():
                now = 0.0
                for b, o, c in queue:
                    now = max(now, there[z].get((b, o, c), far)) + size[c]
                    to = {"up": z + 1, "down": z - 1, "side": z}[name]
                    key = (b, 1 - o if name == "side" else o, c)
                    there[to][key] = now
    result = []
    for z in range(length):
        events = []
        for name, queue in queues[z].items():
            key = 0.0
            for at, (b, o, c) in enumerate(queue):
                key = max(key, there[z][b, o, c])
                events.append((key, at, name, b, o, c))
        assert max(e[0] for e in events) < far
        result.append((sorted(events), there[z]))
    return result


def gather_kernel(
    n_zero, n_model,
    w_q, w_k, w_v, l_q, l_k, l_v, h_q, h_k, h_v, n_a, n_b,
    s_q, s_k, s_v, factors, norms,
    w_vm, h_vm, l_vm, lows, raws, sums, scales, n_vm,
    send_sem, recv_sem, load_sem, sum_sem, norm_sem, ready_sem,
):
    w, low, high = (w_q, w_k, w_v), (l_q, l_k, l_v), (h_q, h_k, h_v)
    served = (s_q, s_k, s_v)
    length = n_zero // COLUMNS
    zero, model = lax.axis_index("zero"), lax.axis_index("model")
    place, column = zero // COLUMNS, zero % COLUMNS
    rows, width = w_q.shape
    rank = l_q.shape[0]
    quarter = rows // 4
    raw_rows = raws.shape[0] // n_zero
    me = zero * n_model + model
    orders = order_of(length)

    barrier = pltpu.get_barrier_semaphore()
    partners = [(zero, lax.rem(model + k, n_model)) for k in range(1, n_model)]
    partners.append((place * COLUMNS + 1 - column, model))
    for to in partners:
        pl.semaphore_signal(barrier, inc=1, device_id=to, device_id_type=MESH)

    @pl.when(place > 0)
    def _():
        pl.semaphore_signal(barrier, inc=1, device_id=(zero - COLUMNS, model), device_id_type=MESH)

    @pl.when(place < length - 1)
    def _():
        pl.semaphore_signal(barrier, inc=1, device_id=(zero + COLUMNS, model), device_id_type=MESH)

    for i, (refs, into) in enumerate(((low, l_vm), (w, w_vm), (high, h_vm), ((n_a, n_b), n_vm))):
        for m, ref in enumerate(refs):
            pltpu.make_async_copy(ref, into.at[m], load_sem.at[i]).start()

    def block_at(b, o):
        return b * COLUMNS + (column if o == 0 else 1 - column)

    def landing(block, c):
        if c == LOW:
            return lows.at[block]
        if c == NORM:
            return norms.at[pl.ds(block * n_model, n_model)]
        m, first, many = PARTS[c]
        ref, tall = (raws, raw_rows) if c < RAW else (served[m], rows)
        first = pl.multiple_of(block * tall, quarter) + first * quarter
        return ref.at[pl.ds(pl.multiple_of(first, quarter), many * quarter)]

    def taken(ref, sem):
        pltpu.make_async_copy(ref, ref, sem).wait()

    def group_of(name, c):
        if c in (LOW, NORM):
            return 6 + c - LOW
        return PARTS[c][0] + 3 * (name == "side")

    def arrival(block, at, c):
        return recv_sem.at[lax.rem(block - at + n_zero - 1, n_zero), c]

    def copy_of(z, name, b, o, c):
        block = block_at(b, o)
        target = {
            "up": (z + 1) * COLUMNS + column,
            "down": (z - 1) * COLUMNS + column,
            "side": z * COLUMNS + 1 - column,
        }[name]
        source = landing(block, c)
        if b == z and o == 0:
            if c < RAW:
                m, first, many = PARTS[c]
                source = w[m].at[pl.ds(first * quarter, many * quarter)]
            if c == LOW:
                source = l_q.at[:, pl.ds(0, raw_rows)]
        return pltpu.make_async_remote_copy(
            src_ref=source,
            dst_ref=landing(block, c),
            send_sem=send_sem.at[group_of(name, c)],
            recv_sem=arrival(block, target, c),
            device_id=(target, model),
            device_id_type=MESH,
        )

    def arrive(b, o, c):
        block = block_at(b, o)
        taken(landing(block, c), arrival(block, zero, c))

    def send_own(z, pieces):
        for key, at, name, b, o, c in orders[z][0]:
            if b == z and o == 0 and c in pieces:
                copy_of(z, name, b, o, c).start()

    def send_all(pieces):
        for z in range(length):

            @pl.when(place == z)
            def _(z=z):
                send_own(z, pieces)

    def ready(z, way):
        pl.semaphore_signal(
            ready_sem.at[way], inc=1, device_id=(zero + (1 - 2 * way) * COLUMNS, model), device_id_type=MESH
        )

    for z in range(length):

        @pl.when(place == z)
        def _(z=z):
            pl.semaphore_wait(barrier, len(partners) + (z > 0) + (z < length - 1))
            send_own(z, (LOW, *range(FIRST)))
            for way in (0, 1):
                if (length - 1 - z, z)[way] and not (z, length - 1 - z)[way]:
                    ready(z, way)

    def relay(step):
        for z in range(length):
            way = step if z < length // 2 else 1 - step

            @pl.when(place == z)
            def _(z=z, way=way):
                if (z, length - 1 - z)[way]:
                    pl.semaphore_wait(ready_sem.at[way], 1)
                    if (length - 1 - z, z)[way]:
                        ready(z, way)

    for i, into in enumerate((l_vm, w_vm, h_vm, n_vm)):
        taken(into, load_sem.at[i])

    def whole_of(m, low_ref, source, at):
        mixed = lax.dot_general(
            low_ref[:, at], h_vm[m], (((0,), (0,)), ((), ())), preferred_element_type=jnp.float32
        )
        return source[at, :].astype(jnp.float32) + mix_rate * mixed

    tile = 128
    for m in range(3):

        def add(i, total, m=m):
            at = pl.ds(pl.multiple_of(i * tile, tile), tile)
            whole = whole_of(m, l_vm.at[m], w_vm.at[m], at)
            return total + jnp.sum(jnp.abs(whole).reshape(tile // 8, 8, width), axis=0)

        total = lax.fori_loop(0, rows // tile, add, jnp.zeros((8, width), jnp.float32))
        sums[zero, :, m * width : (m + 1) * width] = jnp.sum(total, axis=0, keepdims=True)
        if m < 2:
            relay(m)
    norms[pl.ds(me, 1)] = (n_vm[0] + n_vm[1])[None]

    def sum_copy(k):
        to = lax.rem(zero + k, n_zero)
        return pltpu.make_async_remote_copy(
            src_ref=sums.at[zero],
            dst_ref=sums.at[zero],
            send_sem=sum_sem.at[0],
            recv_sem=sum_sem.at[1],
            device_id=(to, model),
            device_id_type=MESH,
        )

    def norm_copy(k):
        return pltpu.make_async_remote_copy(
            src_ref=norms.at[me],
            dst_ref=norms.at[me],
            send_sem=norm_sem.at[0],
            recv_sem=norm_sem.at[1],
            device_id=partners[k - 1],
            device_id_type=MESH,
        )

    for k in range(1, n_zero):
        sum_copy(k).start()
    send_all(tuple(range(FIRST, RAW)))
    for k in range(1, n_model):
        norm_copy(k).start()

    taken(sums.at[pl.ds(0, n_zero - 1)], sum_sem.at[1])
    total = sums[0]
    for b in range(1, n_zero):
        total = total + sums[b]
    factor = total / (rows * n_zero)
    factors[...] = factor
    scales[...] = 1.0 / factor

    def finish(m, block, low_ref, source, start, many):
        base = pl.multiple_of(block * rows, rows)

        def step(i, carry):
            first = pl.multiple_of(start + i * tile, tile)
            whole = whole_of(m, low_ref, source, pl.ds(first, tile))
            to = pl.ds(pl.multiple_of(base + first, tile), tile)
            served[m][to, :] = (whole * scales[:, m * width : (m + 1) * width]).astype(s_q.dtype)
            return carry

        lax.fori_loop(0, many // tile, step, 0)

    def finish_own(m, start, many):
        finish(m, zero, l_vm.at[m], w_vm.at[m], start, many)

    finish_own(0, raw_rows, rows - raw_rows)
    finish_own(1, 0, rows)
    send_all(tuple(c for c in range(RAW, PIECES) if PARTS[c][0] == 0))
    finish_own(2, 0, rows)
    send_all(tuple(c for c in range(RAW, PIECES) if PARTS[c][0] == 1))
    finish_own(0, 0, raw_rows)
    send_all(tuple(c for c in range(RAW, PIECES) if PARTS[c][0] == 2))
    taken(norms.at[pl.ds(0, n_model - 1)], norm_sem.at[1])

    for z in range(length):

        @pl.when(place == z)
        def _(z=z):
            send_own(z, (NORM,))
            events, there = orders[z]
            items = [(key, 0, at, name, b, o, c) for key, at, name, b, o, c in events]
            for b in range(length):
                for o in range(COLUMNS):
                    if (b, o) != (z, 0):
                        when = max(there[b, o, c] for c in (*range(RAW), LOW))
                        items.append((when, 1, 0, "", b, o, 0))
            seen = set()

            def need(b, o, c):
                if (b, o) != (z, 0) and (b, o, c) not in seen:
                    seen.add((b, o, c))
                    arrive(b, o, c)

            for _, kind, at, name, b, o, c in sorted(items):
                if kind == 0:
                    if (b, o) != (z, 0):
                        need(b, o, c)
                        copy_of(z, name, b, o, c).start()
                    continue
                for piece in (*range(RAW), LOW):
                    need(b, o, piece)
                block = block_at(b, o)
                raw = raws.at[pl.ds(pl.multiple_of(block * raw_rows, raw_rows), raw_rows)]
                finish(0, block, lows.at[block], raw, 0, raw_rows)
            for b in range(length):
                for o in range(COLUMNS):
                    for c in range(PIECES + 2):
                        need(b, o, c)
            sent = [0] * 8
            for key, at, name, b, o, c in events:
                sent[group_of(name, c)] += 1 if c in (LOW, NORM) else PARTS[c][2] * quarter
            sent[7] *= n_model
            for i, many in enumerate(sent):
                if many:
                    taken((lows, norms)[i - 6].at[pl.ds(0, many)] if i > 5 else s_q.at[pl.ds(0, many)], send_sem.at[i])

    taken(sums.at[pl.ds(0, n_zero - 1)], sum_sem.at[0])
    taken(norms.at[pl.ds(0, n_model - 1)], norm_sem.at[0])


def write_kernel(s_q, s_k, s_v, factors, norms, o_q, o_k, o_v, f_q, f_k, f_v, norm, norm_vm, sem):
    rows = s_q.shape[0] // WRITES
    width = s_q.shape[1]
    copies = []
    for m, (s, o) in enumerate(((s_q, o_q), (s_k, o_k), (s_v, o_v))):
        for i in range(WRITES):
            part = pl.ds(i * rows, rows)
            copies.append((s.at[part], o.at[part]))
    for m, f in enumerate((f_q, f_k, f_v)):
        copies.append((factors.at[:, pl.ds(m * width, width)], f))
    copies.append((norm_vm, norm))
    copies = [pltpu.make_async_copy(s, o, sem.at[i]) for i, (s, o) in enumerate(copies)]
    for copy in copies[:-1]:
        copy.start()
    norm_vm[...] = norms[...].reshape(norm.shape).astype(norm.dtype)
    copies[-1].start()
    for copy in copies:
        copy.wait()


def on_lines(n_zero, n_model, w_q, l_q, h_q, w_k, l_k, h_k, w_v, l_v, h_v, n_a, n_b):
    rows, width = w_q.shape
    rank = l_q.shape[1]
    d_model = rows * n_zero
    count = n_zero * n_model
    share = n_a.shape[0]
    raw_rows = sum(part[2] for part in PARTS[:RAW]) * rows // 4
    f32, bf16 = jnp.float32, jnp.bfloat16
    shape = jax.ShapeDtypeStruct
    anywhere = pl.BlockSpec(memory_space=pl.ANY)
    inside = pl.BlockSpec(memory_space=pltpu.VMEM)
    dma = pltpu.SemaphoreType.DMA
    tall = (d_model, width)
    s_q, s_k, s_v, factors, norms = pl.pallas_call(
        functools.partial(gather_kernel, n_zero, n_model),
        out_shape=(pltpu.VMEM(tall, bf16),) * 3
        + (pltpu.VMEM((1, 3 * width), f32), pltpu.VMEM((count, 1, share), f32)),
        in_specs=[anywhere] * 11,
        out_specs=(inside,) * 5,
        scratch_shapes=[
            pltpu.VMEM((3, rows, width), bf16),
            pltpu.VMEM((3, rank, width), bf16),
            pltpu.VMEM((3, rank, rows), bf16),
            pltpu.VMEM((n_zero, rank, raw_rows), bf16),
            pltpu.VMEM((n_zero * raw_rows, width), bf16),
            pltpu.VMEM((n_zero, 1, 3 * width), f32),
            pltpu.VMEM((1, 3 * width), f32),
            pltpu.VMEM((2, 1, share), f32),
            dma((8,)),
            dma((n_zero - 1, PIECES + 2)),
            dma((4,)),
            dma((2,)),
            dma((2,)),
            pltpu.SemaphoreType.REGULAR((2,)),
        ],
        compiler_params=pltpu.CompilerParams(
            collective_id=0, has_side_effects=True, vmem_limit_bytes=VMEM_MOST - 3 * d_model * width * 2 - SPARE
        ),
    )(w_q, w_k, w_v, l_q.T, l_k.T, l_v.T, h_q, h_k, h_v, n_a.reshape(1, share), n_b.reshape(1, share))
    *served, f_q, f_k, f_v, norm = pl.pallas_call(
        write_kernel,
        out_shape=(shape(tall, bf16),) * 3 + (shape((1, width), f32),) * 3 + (shape((count, share), bf16),),
        in_specs=[anywhere] * 3 + [inside] * 2,
        out_specs=(anywhere,) * 7,
        scratch_shapes=[pltpu.VMEM((count, share), bf16), dma((3 * WRITES + 4,))],
        compiler_params=pltpu.CompilerParams(
            vmem_limit_bytes=4 * 1024 * 1024
        ),
    )(s_q, s_k, s_v, factors, norms)
    return (*served, f_q.reshape(width), f_k.reshape(width), f_v.reshape(width), norm.reshape(count * share))


def plain(n_zero, n_model, w_q, l_q, h_q, w_k, l_k, h_k, w_v, l_v, h_v, n_a, n_b):
    d_model = w_q.shape[0] * n_zero
    wholes = [
        w.astype(jnp.float32) + mix_rate * jnp.dot(l, h, preferred_element_type=jnp.float32)
        for w, l, h in ((w_q, l_q, h_q), (w_k, l_k, h_k), (w_v, l_v, h_v))
    ]
    totals = lax.psum([jnp.sum(jnp.abs(whole), axis=0) for whole in wholes], "zero")
    factors = [total / d_model for total in totals]
    serving = [
        lax.all_gather((whole / factor).astype(jnp.bfloat16), "zero", axis=0, tiled=True)
        for whole, factor in zip(wholes, factors)
    ]
    norm = lax.all_gather(
        (n_a + n_b).astype(jnp.bfloat16), ("zero", "model"), axis=0, tiled=True
    )
    return (*serving, *factors, norm)


def solution(mesh):
    n_zero, n_model = mesh.shape["zero"], mesh.shape["model"]
    lines = n_zero == 2 * n_model
    tall, low, wide = P("zero", "model"), P("zero", None), P(None, "model")
    return jax.shard_map(
        functools.partial(on_lines if lines else plain, n_zero, n_model),
        mesh=mesh,
        in_specs=(tall, low, wide) * 3 + (P(("zero", "model")),) * 2,
        out_specs=(wide,) * 3 + (P("model"),) * 3 + (P(),),
        check_vma=False,
    )
```

```python
import functools

import jax
import jax.numpy as jnp
from jax import lax
from jax.experimental import pallas as pl
from jax.experimental.pallas import tpu as pltpu
from jax.sharding import PartitionSpec as P

MESH = pl.DeviceIdType.MESH
mix_rate = 0.5
VMEM_MOST = 67_043_328
SPARE = 65_536
COLUMNS = 2
PARTS = ((0, 0, 1), (0, 1, 1), (0, 2, 2), (1, 0, 2), (1, 2, 2), (2, 0, 1), (2, 1, 3))
PIECES = len(PARTS)
RAW = 2
LATE = (4, 5, 6)
LAST = 6
CORES = 2
LOW, NORM = PIECES, PIECES + 1
WRITES = 4
FIRST = 1


def last_of(z, core, length):
    end, inner = (0, 1) if z < length // 2 else (length - 1, length - 2)
    if core == 0:
        return (inner, 1) if z == end else None, (inner, 1) if z == inner else None
    return (length - 1 - end, 1) if z == end else None, (length - 1 - end, 0) if z == end else None


def queues_of(z, core, length):
    every = [LOW] + list(range(PIECES)) + [NORM]
    late = list(LATE)
    early = [c for c in every if c not in late]
    out = {"up": [], "down": [], "side": []}
    if z < length - 1:
        out["up"] += [(z - s, 0, c) for s in range(z + 1) for c in every]
        if z == 0:
            out["up"] += [(0, 1, c) for c in every]
        if z == length - 2:
            out["up"] += [(z, 1, c) for c in late]
    if z > 0:
        out["down"] += [(z + s, 0, c) for s in range(length - z) for c in every]
        if z == length - 1:
            out["down"] += [(z, 1, c) for c in every]
        if z == 1:
            out["down"] += [(z, 1, c) for c in late]
    for b in sorted(range(length), key=lambda b: (abs(b - z), b)):
        pieces = every
        if (z, b) in ((0, 1), (length - 1, length - 2)):
            pieces = early
        if (z, b) in ((1, 0), (length - 2, length - 1)):
            pieces = []
        out["side"] += [(b, 0, c) for c in pieces]
    _, handed = last_of(z, core, length)
    if handed:
        name = "side" if core else "down" if z < length // 2 else "up"
        out[name].remove((*handed, LAST))
    return out


def order_of(core, length):
    size = [part[2] / 2 for part in PARTS] + [0.02, 0.01]
    queues = [queues_of(z, core, length) for z in range(length)]
    far = 1e9
    there = [{} for _ in range(length)]
    for z in range(length):
        for c in range(len(size)):
            there[z][z, 0, c] = 0.0
    for _ in range(4 * length):
        for z in range(length):
            for name, queue in queues[z].items():
                now = 0.0
                for b, o, c in queue:
                    now = max(now, there[z].get((b, o, c), far)) + size[c]
                    to = {"up": z + 1, "down": z - 1, "side": z}[name]
                    key = (b, 1 - o if name == "side" else o, c)
                    there[to][key] = now
    result = []
    for z in range(length):
        events = []
        for name, queue in queues[z].items():
            key = 0.0
            for at, (b, o, c) in enumerate(queue):
                key = max(key, there[z][b, o, c])
                events.append((key, at, name, b, o, c))
        assert max(e[0] for e in events) < far
        result.append((sorted(events), there[z]))
    return result


def gather_kernel(
    n_zero, n_model,
    w_q, w_k, w_v, l_q, l_k, l_v, h_q, h_k, h_v, n_a, n_b,
    s_q, s_k, s_v, factors, norms, hand,
    w_vm, h_vm, l_vm, lows, raws, sums, scales, n_vm,
    send_sem, recv_sem, load_sem, sum_sem, norm_sem, ready_sem,
):
    w, low, high = (w_q, w_k, w_v), (l_q, l_k, l_v), (h_q, h_k, h_v)
    served = (s_q, s_k, s_v)
    length = n_zero // COLUMNS
    zero, model = lax.axis_index("zero"), lax.axis_index("model")
    place, column = zero // COLUMNS, zero % COLUMNS
    rows, width = w_q.shape
    rank = l_q.shape[0]
    quarter = rows // 4
    raw_rows = raws.shape[0] // n_zero
    me = zero * n_model + model
    orders = [order_of(core, length) for core in range(CORES)]
    core_at = model % CORES

    barrier = pltpu.get_barrier_semaphore()
    partners = [(zero, lax.rem(model + k, n_model)) for k in range(1, n_model)]
    partners.append((place * COLUMNS + 1 - column, model))
    for to in partners:
        pl.semaphore_signal(barrier, inc=1, device_id=to, device_id_type=MESH)

    @pl.when(place > 0)
    def _():
        pl.semaphore_signal(barrier, inc=1, device_id=(zero - COLUMNS, model), device_id_type=MESH)

    @pl.when(place < length - 1)
    def _():
        pl.semaphore_signal(barrier, inc=1, device_id=(zero + COLUMNS, model), device_id_type=MESH)

    for i, (refs, into) in enumerate(((low, l_vm), (w, w_vm), (high, h_vm), ((n_a, n_b), n_vm))):
        for m, ref in enumerate(refs):
            pltpu.make_async_copy(ref, into.at[m], load_sem.at[i]).start()

    def block_at(b, o):
        return b * COLUMNS + (column if o == 0 else 1 - column)

    def landing(block, c):
        if c == LOW:
            return lows.at[block]
        if c == NORM:
            return norms.at[pl.ds(block * n_model, n_model)]
        m, first, many = PARTS[c]
        ref, tall = (raws, raw_rows) if c < RAW else (served[m], rows)
        first = pl.multiple_of(block * tall, quarter) + first * quarter
        return ref.at[pl.ds(pl.multiple_of(first, quarter), many * quarter)]

    def taken(ref, sem):
        pltpu.make_async_copy(ref, ref, sem).wait()

    def group_of(name, c):
        if c in (LOW, NORM):
            return 6 + c - LOW
        return PARTS[c][0] + 3 * (name == "side")

    def arrival(block, at, c):
        return recv_sem.at[lax.rem(block - at + n_zero - 1, n_zero), c]

    def copy_of(z, name, b, o, c):
        block = block_at(b, o)
        target = {
            "up": (z + 1) * COLUMNS + column,
            "down": (z - 1) * COLUMNS + column,
            "side": z * COLUMNS + 1 - column,
        }[name]
        source = landing(block, c)
        if b == z and o == 0:
            if c < RAW:
                m, first, many = PARTS[c]
                source = w[m].at[pl.ds(first * quarter, many * quarter)]
            if c == LOW:
                source = l_q.at[:, pl.ds(0, raw_rows)]
        return pltpu.make_async_remote_copy(
            src_ref=source,
            dst_ref=landing(block, c),
            send_sem=send_sem.at[group_of(name, c)],
            recv_sem=arrival(block, target, c),
            device_id=(target, model),
            device_id_type=MESH,
        )

    def arrive(b, o, c):
        block = block_at(b, o)
        taken(landing(block, c), arrival(block, zero, c))

    def send_own(z, pieces):
        for key, at, name, b, o, c in orders[0][z][0]:
            if b == z and o == 0 and c in pieces:
                copy_of(z, name, b, o, c).start()

    def send_all(pieces):
        for z in range(length):

            @pl.when(place == z)
            def _(z=z):
                send_own(z, pieces)

    def ready(z, way):
        pl.semaphore_signal(
            ready_sem.at[way], inc=1, device_id=(zero + (1 - 2 * way) * COLUMNS, model), device_id_type=MESH
        )

    for z in range(length):

        @pl.when(place == z)
        def _(z=z):
            pl.semaphore_wait(barrier, len(partners) + (z > 0) + (z < length - 1))
            send_own(z, (LOW, *range(FIRST)))
            for way in (0, 1):
                if (length - 1 - z, z)[way] and not (z, length - 1 - z)[way]:
                    ready(z, way)

    def relay(step):
        for z in range(length):
            way = step if z < length // 2 else 1 - step

            @pl.when(place == z)
            def _(z=z, way=way):
                if (z, length - 1 - z)[way]:
                    pl.semaphore_wait(ready_sem.at[way], 1)
                    if (length - 1 - z, z)[way]:
                        ready(z, way)

    for i, into in enumerate((l_vm, w_vm, h_vm, n_vm)):
        taken(into, load_sem.at[i])

    def whole_of(m, low_ref, source, at):
        mixed = lax.dot_general(
            low_ref[:, at], h_vm[m], (((0,), (0,)), ((), ())), preferred_element_type=jnp.float32
        )
        return source[at, :].astype(jnp.float32) + mix_rate * mixed

    tile = 128
    for m in range(3):

        def add(i, total, m=m):
            at = pl.ds(pl.multiple_of(i * tile, tile), tile)
            whole = whole_of(m, l_vm.at[m], w_vm.at[m], at)
            return total + jnp.sum(jnp.abs(whole).reshape(tile // 8, 8, width), axis=0)

        total = lax.fori_loop(0, rows // tile, add, jnp.zeros((8, width), jnp.float32))
        sums[zero, :, m * width : (m + 1) * width] = jnp.sum(total, axis=0, keepdims=True)
        if m < 2:
            relay(m)
    norms[pl.ds(me, 1)] = (n_vm[0] + n_vm[1])[None]

    def sum_copy(k):
        to = lax.rem(zero + k, n_zero)
        return pltpu.make_async_remote_copy(
            src_ref=sums.at[zero],
            dst_ref=sums.at[zero],
            send_sem=sum_sem.at[0],
            recv_sem=sum_sem.at[1],
            device_id=(to, model),
            device_id_type=MESH,
        )

    def norm_copy(k):
        return pltpu.make_async_remote_copy(
            src_ref=norms.at[me],
            dst_ref=norms.at[me],
            send_sem=norm_sem.at[0],
            recv_sem=norm_sem.at[1],
            device_id=partners[k - 1],
            device_id_type=MESH,
        )

    for k in range(1, n_zero):
        sum_copy(k).start()
    send_all(tuple(range(FIRST, RAW)))
    for k in range(1, n_model):
        norm_copy(k).start()

    taken(sums.at[pl.ds(0, n_zero - 1)], sum_sem.at[1])
    total = sums[0]
    for b in range(1, n_zero):
        total = total + sums[b]
    factor = total / (rows * n_zero)
    factors[...] = factor
    scales[...] = 1.0 / factor

    def finish(m, block, low_ref, source, start, many):
        base = pl.multiple_of(block * rows, rows)

        def step(i, carry):
            first = pl.multiple_of(start + i * tile, tile)
            whole = whole_of(m, low_ref, source, pl.ds(first, tile))
            to = pl.ds(pl.multiple_of(base + first, tile), tile)
            served[m][to, :] = (whole * scales[:, m * width : (m + 1) * width]).astype(s_q.dtype)
            return carry

        lax.fori_loop(0, many // tile, step, 0)

    def finish_own(m, start, many):
        finish(m, zero, l_vm.at[m], w_vm.at[m], start, many)

    finish_own(0, raw_rows, rows - raw_rows)
    finish_own(1, 0, rows)
    send_all(tuple(c for c in range(RAW, PIECES) if PARTS[c][0] == 0))
    finish_own(2, 0, rows)
    send_all(tuple(c for c in range(RAW, PIECES) if PARTS[c][0] == 1))
    finish_own(0, 0, raw_rows)
    send_all(tuple(c for c in range(RAW, PIECES) if PARTS[c][0] == 2))
    taken(norms.at[pl.ds(0, n_model - 1)], norm_sem.at[1])

    send_all((NORM,))

    def hand_on(b, o):
        block = block_at(b, o)
        m, first, many = PARTS[LAST]
        base = pl.multiple_of(block * rows, rows) + first * quarter

        def step(i, carry):
            at = pl.multiple_of(i * tile, tile)
            hand[pl.ds(at, tile), :] = served[m][pl.ds(pl.multiple_of(base + at, tile), tile), :]
            return carry

        lax.fori_loop(0, many * quarter // tile, step, 0)

    def serve(z, core):
        events, there = orders[core][z]
        lacking, handed = last_of(z, core, length)
        items = [(key, 0, name, b, o, c) for key, at, name, b, o, c in events]
        for b in range(length):
            for o in range(COLUMNS):
                if (b, o) != (z, 0):
                    when = max(there[b, o, c] for c in (*range(RAW), LOW))
                    items.append((when, 1, "", b, o, 0))
        if handed:
            items.append((there[(*handed, LAST)], 2, "", *handed, LAST))
        seen = {(z, 0, c) for c in range(PIECES + 2)}
        if lacking:
            seen.add((*lacking, LAST))

        def need(b, o, c):
            if (b, o, c) not in seen:
                seen.add((b, o, c))
                arrive(b, o, c)

        for _, kind, name, b, o, c in sorted(items):
            if kind == 0:
                if (b, o) != (z, 0):
                    need(b, o, c)
                    copy_of(z, name, b, o, c).start()
            elif kind == 1:
                for piece in (*range(RAW), LOW):
                    need(b, o, piece)
                block = block_at(b, o)
                raw = raws.at[pl.ds(pl.multiple_of(block * raw_rows, raw_rows), raw_rows)]
                finish(0, block, lows.at[block], raw, 0, raw_rows)
            else:
                need(b, o, c)
                hand_on(b, o)
        for b in range(length):
            for o in range(COLUMNS):
                for c in range(PIECES + 2):
                    need(b, o, c)
        sent = [0] * 8
        for key, at, name, b, o, c in events:
            sent[group_of(name, c)] += 1 if c in (LOW, NORM) else PARTS[c][2] * quarter
        sent[7] *= n_model
        for i, many in enumerate(sent):
            if many:
                taken((lows, norms)[i - 6].at[pl.ds(0, many)] if i > 5 else s_q.at[pl.ds(0, many)], send_sem.at[i])

    for z in range(length):
        for core in range(CORES):
            pl.when((place == z) & (core_at == core))(functools.partial(serve, z, core))

    taken(sums.at[pl.ds(0, n_zero - 1)], sum_sem.at[0])
    taken(norms.at[pl.ds(0, n_model - 1)], norm_sem.at[0])


def write_kernel(s_q, s_k, s_v, factors, norms, o_q, o_k, o_v, f_q, f_k, f_v, norm, norm_vm, sem):
    rows = s_q.shape[0] // WRITES
    width = s_q.shape[1]
    copies = []
    for m, (s, o) in enumerate(((s_q, o_q), (s_k, o_k), (s_v, o_v))):
        for i in range(WRITES):
            part = pl.ds(i * rows, rows)
            copies.append((s.at[part], o.at[part]))
    for m, f in enumerate((f_q, f_k, f_v)):
        copies.append((factors.at[:, pl.ds(m * width, width)], f))
    copies.append((norm_vm, norm))
    copies = [pltpu.make_async_copy(s, o, sem.at[i]) for i, (s, o) in enumerate(copies)]
    for copy in copies[:-1]:
        copy.start()
    norm_vm[...] = norms[...].reshape(norm.shape).astype(norm.dtype)
    copies[-1].start()
    for copy in copies:
        copy.wait()


def last_kernel(n_zero, n_model, given, late, out, sem):
    length = n_zero // COLUMNS
    zero, model = lax.axis_index("zero"), lax.axis_index("model")
    place, column, core_at = zero // COLUMNS, zero % COLUMNS, model % CORES
    rows = out.shape[0] // n_zero
    first = PARTS[LAST][1] * (rows // 4)
    for z in (0, length - 1):
        for core in range(CORES):
            lacking, _ = last_of(z, core, length)

            @pl.when((place == z) & (core_at == core))
            def _(b=lacking[0]):
                block = b * COLUMNS + 1 - column
                base = pl.multiple_of(block * rows, rows) + first
                part = out.at[pl.ds(pl.multiple_of(base, rows // 4), late.shape[0])]
                copy = pltpu.make_async_copy(late, part, sem)
                copy.start()
                copy.wait()


def on_lines(n_zero, n_model, w_q, l_q, h_q, w_k, l_k, h_k, w_v, l_v, h_v, n_a, n_b):
    rows, width = w_q.shape
    rank = l_q.shape[1]
    d_model = rows * n_zero
    count = n_zero * n_model
    share = n_a.shape[0]
    raw_rows = sum(part[2] for part in PARTS[:RAW]) * rows // 4
    f32, bf16 = jnp.float32, jnp.bfloat16
    shape = jax.ShapeDtypeStruct
    anywhere = pl.BlockSpec(memory_space=pl.ANY)
    inside = pl.BlockSpec(memory_space=pltpu.VMEM)
    dma = pltpu.SemaphoreType.DMA
    tall = (d_model, width)
    hand_rows = PARTS[LAST][2] * rows // 4
    s_q, s_k, s_v, factors, norms, hand = pl.pallas_call(
        functools.partial(gather_kernel, n_zero, n_model),
        out_shape=(pltpu.VMEM(tall, bf16),) * 3
        + (pltpu.VMEM((1, 3 * width), f32), pltpu.VMEM((count, 1, share), f32), pltpu.VMEM((hand_rows, width), bf16)),
        in_specs=[anywhere] * 11,
        out_specs=(inside,) * 6,
        scratch_shapes=[
            pltpu.VMEM((3, rows, width), bf16),
            pltpu.VMEM((3, rank, width), bf16),
            pltpu.VMEM((3, rank, rows), bf16),
            pltpu.VMEM((n_zero, rank, raw_rows), bf16),
            pltpu.VMEM((n_zero * raw_rows, width), bf16),
            pltpu.VMEM((n_zero, 1, 3 * width), f32),
            pltpu.VMEM((1, 3 * width), f32),
            pltpu.VMEM((2, 1, share), f32),
            dma((8,)),
            dma((n_zero - 1, PIECES + 2)),
            dma((4,)),
            dma((2,)),
            dma((2,)),
            pltpu.SemaphoreType.REGULAR((2,)),
        ],
        compiler_params=pltpu.CompilerParams(
            collective_id=0, has_side_effects=True, vmem_limit_bytes=VMEM_MOST - 3 * d_model * width * 2 - 8 * hand_rows * width - SPARE
        ),
    )(w_q, w_k, w_v, l_q.T, l_k.T, l_v.T, h_q, h_k, h_v, n_a.reshape(1, share), n_b.reshape(1, share))
    pairs = []
    for zero in range(n_zero):
        for model in range(n_model):
            z, column, core = zero // COLUMNS, zero % COLUMNS, model % CORES
            lacking, _ = last_of(z, core, n_zero // COLUMNS)
            if lacking:
                giver = (z * COLUMNS + 1 - column) if core else lacking[0] * COLUMNS + column
                pairs.append((giver * n_model + model, zero * n_model + model))
    late = lax.ppermute(hand, ("zero", "model"), pairs)
    *served, f_q, f_k, f_v, norm = pl.pallas_call(
        write_kernel,
        out_shape=(shape(tall, bf16),) * 3 + (shape((1, width), f32),) * 3 + (shape((count, share), bf16),),
        in_specs=[anywhere] * 3 + [inside] * 2,
        out_specs=(anywhere,) * 7,
        scratch_shapes=[pltpu.VMEM((count, share), bf16), dma((3 * WRITES + 4,))],
        compiler_params=pltpu.CompilerParams(
            vmem_limit_bytes=4 * 1024 * 1024
        ),
        cost_estimate=pl.CostEstimate(flops=10**9, bytes_accessed=12 * d_model * width, transcendentals=0),
    )(s_q, s_k, s_v, factors, norms)
    served[2] = pl.pallas_call(
        functools.partial(last_kernel, n_zero, n_model),
        out_shape=shape(tall, bf16),
        in_specs=[anywhere] * 2,
        out_specs=anywhere,
        scratch_shapes=[dma],
        input_output_aliases={0: 0},
        compiler_params=pltpu.CompilerParams(vmem_limit_bytes=1024 * 1024),
    )(served[2], late)
    return (*served, f_q.reshape(width), f_k.reshape(width), f_v.reshape(width), norm.reshape(count * share))


def plain(n_zero, n_model, w_q, l_q, h_q, w_k, l_k, h_k, w_v, l_v, h_v, n_a, n_b):
    d_model = w_q.shape[0] * n_zero
    wholes = [
        w.astype(jnp.float32) + mix_rate * jnp.dot(l, h, preferred_element_type=jnp.float32)
        for w, l, h in ((w_q, l_q, h_q), (w_k, l_k, h_k), (w_v, l_v, h_v))
    ]
    totals = lax.psum([jnp.sum(jnp.abs(whole), axis=0) for whole in wholes], "zero")
    factors = [total / d_model for total in totals]
    serving = [
        lax.all_gather((whole / factor).astype(jnp.bfloat16), "zero", axis=0, tiled=True)
        for whole, factor in zip(wholes, factors)
    ]
    norm = lax.all_gather(
        (n_a + n_b).astype(jnp.bfloat16), ("zero", "model"), axis=0, tiled=True
    )
    return (*serving, *factors, norm)


def solution(mesh):
    n_zero, n_model = mesh.shape["zero"], mesh.shape["model"]
    lines = n_zero == 2 * n_model
    tall, low, wide = P("zero", "model"), P("zero", None), P(None, "model")
    return jax.shard_map(
        functools.partial(on_lines if lines else plain, n_zero, n_model),
        mesh=mesh,
        in_specs=(tall, low, wide) * 3 + (P(("zero", "model")),) * 2,
        out_specs=(wide,) * 3 + (P("model"),) * 3 + (P(),),
        check_vma=False,
    )
```

```python
import functools

import jax
import jax.numpy as jnp
from jax import lax
from jax.experimental import pallas as pl
from jax.experimental.pallas import tpu as pltpu
from jax.sharding import PartitionSpec as P

MESH = pl.DeviceIdType.MESH
mix_rate = 0.5
VMEM_MOST = 67_043_328
SPARE = 65_536
COLUMNS = 2
PARTS = ((0, 0, 1), (0, 1, 1), (0, 2, 2), (1, 0, 2), (1, 2, 2), (2, 0, 1), (2, 1, 3))
PIECES = len(PARTS)
RAW = 2
LATE = (4, 5, 6)
LAST = 6
CORES = 2
LOW, NORM = PIECES, PIECES + 1
WRITES = 4
FIRST = 1


def last_of(z, core, length):
    end, inner = (0, 1) if z < length // 2 else (length - 1, length - 2)
    if core == 0:
        return (inner, 1) if z == end else None, (inner, 1) if z == inner else None
    return (length - 1 - end, 1) if z == end else None, (length - 1 - end, 0) if z == end else None


def queues_of(z, core, length):
    every = [LOW, *range(RAW + 1), NORM, *range(RAW + 1, PIECES)]
    late = list(LATE)
    early = [c for c in every if c not in late]
    out = {"up": [], "down": [], "side": []}
    if z < length - 1:
        out["up"] += [(z - s, 0, c) for s in range(z + 1) for c in every]
        if z == 0:
            out["up"] += [(0, 1, c) for c in every]
        if z == length - 2:
            out["up"] += [(z, 1, c) for c in late]
    if z > 0:
        out["down"] += [(z + s, 0, c) for s in range(length - z) for c in every]
        if z == length - 1:
            out["down"] += [(z, 1, c) for c in every]
        if z == 1:
            out["down"] += [(z, 1, c) for c in late]
    for b in sorted(range(length), key=lambda b: (abs(b - z), b)):
        pieces = every
        if (z, b) in ((0, 1), (length - 1, length - 2)):
            pieces = early
        if (z, b) in ((1, 0), (length - 2, length - 1)):
            pieces = []
        out["side"] += [(b, 0, c) for c in pieces]
    _, handed = last_of(z, core, length)
    if handed:
        name = "side" if core else "down" if z < length // 2 else "up"
        out[name].remove((*handed, LAST))
    return out


def order_of(core, length):
    size = [part[2] / 2 for part in PARTS] + [0.02, 0.01]
    queues = [queues_of(z, core, length) for z in range(length)]
    far = 1e9
    there = [{} for _ in range(length)]
    for z in range(length):
        for c in range(len(size)):
            there[z][z, 0, c] = 0.0
    for _ in range(4 * length):
        for z in range(length):
            for name, queue in queues[z].items():
                now = 0.0
                for b, o, c in queue:
                    now = max(now, there[z].get((b, o, c), far)) + size[c]
                    to = {"up": z + 1, "down": z - 1, "side": z}[name]
                    key = (b, 1 - o if name == "side" else o, c)
                    there[to][key] = now
    result = []
    for z in range(length):
        events = []
        for name, queue in queues[z].items():
            key = 0.0
            for at, (b, o, c) in enumerate(queue):
                key = max(key, there[z][b, o, c])
                events.append((key, at, name, b, o, c))
        assert max(e[0] for e in events) < far
        result.append((sorted(events), there[z]))
    return result


def gather_kernel(
    n_zero, n_model,
    w_q, w_k, w_v, l_q, l_k, l_v, h_q, h_k, h_v, n_a, n_b,
    s_q, s_k, s_v, factors, norms, hand,
    w_vm, h_vm, l_vm, lows, raws, sums, scales, n_vm,
    send_sem, recv_sem, load_sem, sum_sem, norm_sem, ready_sem,
):
    w, low, high = (w_q, w_k, w_v), (l_q, l_k, l_v), (h_q, h_k, h_v)
    served = (s_q, s_k, s_v)
    length = n_zero // COLUMNS
    zero, model = lax.axis_index("zero"), lax.axis_index("model")
    place, column = zero // COLUMNS, zero % COLUMNS
    rows, width = w_q.shape
    rank = l_q.shape[0]
    quarter = rows // 4
    raw_rows = raws.shape[0] // n_zero
    me = zero * n_model + model
    orders = [order_of(core, length) for core in range(CORES)]
    core_at = model % CORES

    barrier = pltpu.get_barrier_semaphore()
    partners = [(zero, lax.rem(model + k, n_model)) for k in range(1, n_model)]
    partners.append((place * COLUMNS + 1 - column, model))
    for to in partners:
        pl.semaphore_signal(barrier, inc=1, device_id=to, device_id_type=MESH)

    @pl.when(place > 0)
    def _():
        pl.semaphore_signal(barrier, inc=1, device_id=(zero - COLUMNS, model), device_id_type=MESH)

    @pl.when(place < length - 1)
    def _():
        pl.semaphore_signal(barrier, inc=1, device_id=(zero + COLUMNS, model), device_id_type=MESH)

    for i, (refs, into) in enumerate(((low, l_vm), (w, w_vm), (high, h_vm), ((n_a, n_b), n_vm))):
        for m, ref in enumerate(refs):
            pltpu.make_async_copy(ref, into.at[m], load_sem.at[i]).start()

    def block_at(b, o):
        return b * COLUMNS + (column if o == 0 else 1 - column)

    def landing(block, c):
        if c == LOW:
            return lows.at[block]
        if c == NORM:
            return norms.at[pl.ds(block * n_model, n_model)]
        m, first, many = PARTS[c]
        ref, tall = (raws, raw_rows) if c < RAW else (served[m], rows)
        first = pl.multiple_of(block * tall, quarter) + first * quarter
        return ref.at[pl.ds(pl.multiple_of(first, quarter), many * quarter)]

    def taken(ref, sem):
        pltpu.make_async_copy(ref, ref, sem).wait()

    def group_of(name, c):
        if c in (LOW, NORM):
            return 6 + c - LOW
        return PARTS[c][0] + 3 * (name == "side")

    def arrival(block, at, c):
        return recv_sem.at[lax.rem(block - at + n_zero - 1, n_zero), c]

    def copy_of(z, name, b, o, c):
        block = block_at(b, o)
        target = {
            "up": (z + 1) * COLUMNS + column,
            "down": (z - 1) * COLUMNS + column,
            "side": z * COLUMNS + 1 - column,
        }[name]
        source = landing(block, c)
        if b == z and o == 0:
            if c < RAW:
                m, first, many = PARTS[c]
                source = w[m].at[pl.ds(first * quarter, many * quarter)]
            if c == LOW:
                source = l_q.at[:, pl.ds(0, raw_rows)]
        return pltpu.make_async_remote_copy(
            src_ref=source,
            dst_ref=landing(block, c),
            send_sem=send_sem.at[group_of(name, c)],
            recv_sem=arrival(block, target, c),
            device_id=(target, model),
            device_id_type=MESH,
        )

    def arrive(b, o, c):
        block = block_at(b, o)
        taken(landing(block, c), arrival(block, zero, c))

    def send_own(z, pieces):
        for key, at, name, b, o, c in orders[0][z][0]:
            if b == z and o == 0 and c in pieces:
                copy_of(z, name, b, o, c).start()

    def send_all(pieces):
        for z in range(length):

            @pl.when(place == z)
            def _(z=z):
                send_own(z, pieces)

    def ready(z, way):
        pl.semaphore_signal(
            ready_sem.at[way], inc=1, device_id=(zero + (1 - 2 * way) * COLUMNS, model), device_id_type=MESH
        )

    for z in range(length):

        @pl.when(place == z)
        def _(z=z):
            pl.semaphore_wait(barrier, len(partners) + (z > 0) + (z < length - 1))
            send_own(z, (LOW, *range(FIRST)))
            for way in (0, 1):
                if (length - 1 - z, z)[way] and not (z, length - 1 - z)[way]:
                    ready(z, way)

    def relay(step):
        for z in range(length):
            way = step if z < length // 2 else 1 - step

            @pl.when(place == z)
            def _(z=z, way=way):
                if (z, length - 1 - z)[way]:
                    pl.semaphore_wait(ready_sem.at[way], 1)
                    if (length - 1 - z, z)[way]:
                        ready(z, way)

    for i, into in enumerate((l_vm, w_vm, h_vm, n_vm)):
        taken(into, load_sem.at[i])

    def whole_of(m, low_ref, source, at):
        mixed = lax.dot_general(
            low_ref[:, at], h_vm[m], (((0,), (0,)), ((), ())), preferred_element_type=jnp.float32
        )
        return source[at, :].astype(jnp.float32) + mix_rate * mixed

    tile = 128
    for m in range(3):

        def add(i, total, m=m):
            at = pl.ds(pl.multiple_of(i * tile, tile), tile)
            whole = whole_of(m, l_vm.at[m], w_vm.at[m], at)
            return total + jnp.sum(jnp.abs(whole).reshape(tile // 8, 8, width), axis=0)

        total = lax.fori_loop(0, rows // tile, add, jnp.zeros((8, width), jnp.float32))
        sums[zero, :, m * width : (m + 1) * width] = jnp.sum(total, axis=0, keepdims=True)
        if m < 2:
            relay(m)
    norms[pl.ds(me, 1)] = (n_vm[0] + n_vm[1])[None]

    def sum_copy(k):
        to = lax.rem(zero + k, n_zero)
        return pltpu.make_async_remote_copy(
            src_ref=sums.at[zero],
            dst_ref=sums.at[zero],
            send_sem=sum_sem.at[0],
            recv_sem=sum_sem.at[1],
            device_id=(to, model),
            device_id_type=MESH,
        )

    def norm_copy(k):
        return pltpu.make_async_remote_copy(
            src_ref=norms.at[me],
            dst_ref=norms.at[me],
            send_sem=norm_sem.at[0],
            recv_sem=norm_sem.at[1],
            device_id=partners[k - 1],
            device_id_type=MESH,
        )

    for k in range(1, n_zero):
        sum_copy(k).start()
    send_all(tuple(range(FIRST, RAW)))
    for k in range(1, n_model):
        norm_copy(k).start()

    taken(sums.at[pl.ds(0, n_zero - 1)], sum_sem.at[1])
    total = sums[0]
    for b in range(1, n_zero):
        total = total + sums[b]
    factor = total / (rows * n_zero)
    factors[...] = factor
    scales[...] = 1.0 / factor

    def finish(m, block, low_ref, source, start, many):
        base = pl.multiple_of(block * rows, rows)

        def step(i, carry):
            first = pl.multiple_of(start + i * tile, tile)
            whole = whole_of(m, low_ref, source, pl.ds(first, tile))
            to = pl.ds(pl.multiple_of(base + first, tile), tile)
            served[m][to, :] = (whole * scales[:, m * width : (m + 1) * width]).astype(s_q.dtype)
            return carry

        lax.fori_loop(0, many // tile, step, 0)

    def finish_own(m, start, many):
        finish(m, zero, l_vm.at[m], w_vm.at[m], start, many)

    finish_own(0, raw_rows, rows - raw_rows)
    finish_own(1, 0, rows)
    taken(norms.at[pl.ds(0, n_model - 1)], norm_sem.at[1])
    send_all((NORM, *(c for c in range(RAW, PIECES) if PARTS[c][0] == 0)))
    finish_own(2, 0, rows)
    send_all(tuple(c for c in range(RAW, PIECES) if PARTS[c][0] == 1))
    finish_own(0, 0, raw_rows)
    send_all(tuple(c for c in range(RAW, PIECES) if PARTS[c][0] == 2))
    def hand_on(b, o):
        block = block_at(b, o)
        m, first, many = PARTS[LAST]
        base = pl.multiple_of(block * rows, rows) + first * quarter

        def step(i, carry):
            at = pl.multiple_of(i * tile, tile)
            hand[pl.ds(at, tile), :] = served[m][pl.ds(pl.multiple_of(base + at, tile), tile), :]
            return carry

        lax.fori_loop(0, many * quarter // tile, step, 0)

    def serve(z, core):
        events, there = orders[core][z]
        lacking, handed = last_of(z, core, length)
        items = [(key, 0, at, name, b, o, c) for key, at, name, b, o, c in events]
        for b in range(length):
            for o in range(COLUMNS):
                if (b, o) != (z, 0):
                    when = max(there[b, o, c] for c in (*range(RAW), LOW))
                    items.append((when, 1, 0, "", b, o, 0))
        if handed:
            items.append((there[(*handed, LAST)], 2, 0, "", *handed, LAST))
        seen = {(z, 0, c) for c in range(PIECES + 2)}
        if lacking:
            seen.add((*lacking, LAST))

        def need(b, o, c):
            if (b, o, c) not in seen:
                seen.add((b, o, c))
                arrive(b, o, c)

        for _, kind, _, name, b, o, c in sorted(items):
            if kind == 0:
                if (b, o) != (z, 0):
                    need(b, o, c)
                    copy_of(z, name, b, o, c).start()
            elif kind == 1:
                for piece in (*range(RAW), LOW):
                    need(b, o, piece)
                block = block_at(b, o)
                raw = raws.at[pl.ds(pl.multiple_of(block * raw_rows, raw_rows), raw_rows)]
                finish(0, block, lows.at[block], raw, 0, raw_rows)
            else:
                need(b, o, c)
                hand_on(b, o)
        for b in range(length):
            for o in range(COLUMNS):
                for c in range(PIECES + 2):
                    need(b, o, c)
        sent = [0] * 8
        for key, at, name, b, o, c in events:
            sent[group_of(name, c)] += 1 if c in (LOW, NORM) else PARTS[c][2] * quarter
        sent[7] *= n_model
        for i, many in enumerate(sent):
            if many:
                taken((lows, norms)[i - 6].at[pl.ds(0, many)] if i > 5 else s_q.at[pl.ds(0, many)], send_sem.at[i])

    for z in range(length):
        for core in range(CORES):
            pl.when((place == z) & (core_at == core))(functools.partial(serve, z, core))

    taken(sums.at[pl.ds(0, n_zero - 1)], sum_sem.at[0])
    taken(norms.at[pl.ds(0, n_model - 1)], norm_sem.at[0])


def write_kernel(s_q, s_k, s_v, factors, norms, o_q, o_k, o_v, f_q, f_k, f_v, norm, norm_vm, sem):
    rows = s_q.shape[0] // WRITES
    width = s_q.shape[1]
    copies = []
    for m, (s, o) in enumerate(((s_q, o_q), (s_k, o_k), (s_v, o_v))):
        for i in range(WRITES):
            part = pl.ds(i * rows, rows)
            copies.append((s.at[part], o.at[part]))
    for m, f in enumerate((f_q, f_k, f_v)):
        copies.append((factors.at[:, pl.ds(m * width, width)], f))
    copies.append((norm_vm, norm))
    copies = [pltpu.make_async_copy(s, o, sem.at[i]) for i, (s, o) in enumerate(copies)]
    for copy in copies[:-1]:
        copy.start()
    norm_vm[...] = norms[...].reshape(norm.shape).astype(norm.dtype)
    copies[-1].start()
    for copy in copies:
        copy.wait()


def last_kernel(n_zero, n_model, given, late, out, sem):
    length = n_zero // COLUMNS
    zero, model = lax.axis_index("zero"), lax.axis_index("model")
    place, column, core_at = zero // COLUMNS, zero % COLUMNS, model % CORES
    rows = out.shape[0] // n_zero
    first = PARTS[LAST][1] * (rows // 4)
    for z in (0, length - 1):
        for core in range(CORES):
            lacking, _ = last_of(z, core, length)

            @pl.when((place == z) & (core_at == core))
            def _(b=lacking[0]):
                block = b * COLUMNS + 1 - column
                base = pl.multiple_of(block * rows, rows) + first
                part = out.at[pl.ds(pl.multiple_of(base, rows // 4), late.shape[0])]
                copy = pltpu.make_async_copy(late, part, sem)
                copy.start()
                copy.wait()


def on_lines(n_zero, n_model, w_q, l_q, h_q, w_k, l_k, h_k, w_v, l_v, h_v, n_a, n_b):
    rows, width = w_q.shape
    rank = l_q.shape[1]
    d_model = rows * n_zero
    count = n_zero * n_model
    share = n_a.shape[0]
    raw_rows = sum(part[2] for part in PARTS[:RAW]) * rows // 4
    f32, bf16 = jnp.float32, jnp.bfloat16
    shape = jax.ShapeDtypeStruct
    anywhere = pl.BlockSpec(memory_space=pl.ANY)
    inside = pl.BlockSpec(memory_space=pltpu.VMEM)
    dma = pltpu.SemaphoreType.DMA
    tall = (d_model, width)
    hand_rows = PARTS[LAST][2] * rows // 4
    s_q, s_k, s_v, factors, norms, hand = pl.pallas_call(
        functools.partial(gather_kernel, n_zero, n_model),
        out_shape=(pltpu.VMEM(tall, bf16),) * 3
        + (pltpu.VMEM((1, 3 * width), f32), pltpu.VMEM((count, 1, share), f32), pltpu.VMEM((hand_rows, width), bf16)),
        in_specs=[anywhere] * 11,
        out_specs=(inside,) * 6,
        scratch_shapes=[
            pltpu.VMEM((3, rows, width), bf16),
            pltpu.VMEM((3, rank, width), bf16),
            pltpu.VMEM((3, rank, rows), bf16),
            pltpu.VMEM((n_zero, rank, raw_rows), bf16),
            pltpu.VMEM((n_zero * raw_rows, width), bf16),
            pltpu.VMEM((n_zero, 1, 3 * width), f32),
            pltpu.VMEM((1, 3 * width), f32),
            pltpu.VMEM((2, 1, share), f32),
            dma((8,)),
            dma((n_zero - 1, PIECES + 2)),
            dma((4,)),
            dma((2,)),
            dma((2,)),
            pltpu.SemaphoreType.REGULAR((2,)),
        ],
        compiler_params=pltpu.CompilerParams(
            collective_id=0, has_side_effects=True, vmem_limit_bytes=VMEM_MOST - 3 * d_model * width * 2 - 8 * hand_rows * width - SPARE
        ),
    )(w_q, w_k, w_v, l_q.T, l_k.T, l_v.T, h_q, h_k, h_v, n_a.reshape(1, share), n_b.reshape(1, share))
    pairs = []
    for zero in range(n_zero):
        for model in range(n_model):
            z, column, core = zero // COLUMNS, zero % COLUMNS, model % CORES
            lacking, _ = last_of(z, core, n_zero // COLUMNS)
            if lacking:
                giver = (z * COLUMNS + 1 - column) if core else lacking[0] * COLUMNS + column
                pairs.append((giver * n_model + model, zero * n_model + model))
    late = lax.ppermute(hand, ("zero", "model"), pairs)
    *served, f_q, f_k, f_v, norm = pl.pallas_call(
        write_kernel,
        out_shape=(shape(tall, bf16),) * 3 + (shape((1, width), f32),) * 3 + (shape((count, share), bf16),),
        in_specs=[anywhere] * 3 + [inside] * 2,
        out_specs=(anywhere,) * 7,
        scratch_shapes=[pltpu.VMEM((count, share), bf16), dma((3 * WRITES + 4,))],
        compiler_params=pltpu.CompilerParams(
            vmem_limit_bytes=4 * 1024 * 1024
        ),
        cost_estimate=pl.CostEstimate(flops=10**9, bytes_accessed=12 * d_model * width, transcendentals=0),
    )(s_q, s_k, s_v, factors, norms)
    served[2] = pl.pallas_call(
        functools.partial(last_kernel, n_zero, n_model),
        out_shape=shape(tall, bf16),
        in_specs=[anywhere] * 2,
        out_specs=anywhere,
        scratch_shapes=[dma],
        input_output_aliases={0: 0},
        compiler_params=pltpu.CompilerParams(vmem_limit_bytes=1024 * 1024),
    )(served[2], late)
    return (*served, f_q.reshape(width), f_k.reshape(width), f_v.reshape(width), norm.reshape(count * share))


def plain(n_zero, n_model, w_q, l_q, h_q, w_k, l_k, h_k, w_v, l_v, h_v, n_a, n_b):
    d_model = w_q.shape[0] * n_zero
    wholes = [
        w.astype(jnp.float32) + mix_rate * jnp.dot(l, h, preferred_element_type=jnp.float32)
        for w, l, h in ((w_q, l_q, h_q), (w_k, l_k, h_k), (w_v, l_v, h_v))
    ]
    totals = lax.psum([jnp.sum(jnp.abs(whole), axis=0) for whole in wholes], "zero")
    factors = [total / d_model for total in totals]
    serving = [
        lax.all_gather((whole / factor).astype(jnp.bfloat16), "zero", axis=0, tiled=True)
        for whole, factor in zip(wholes, factors)
    ]
    norm = lax.all_gather(
        (n_a + n_b).astype(jnp.bfloat16), ("zero", "model"), axis=0, tiled=True
    )
    return (*serving, *factors, norm)


def solution(mesh):
    n_zero, n_model = mesh.shape["zero"], mesh.shape["model"]
    lines = n_zero == 2 * n_model
    tall, low, wide = P("zero", "model"), P("zero", None), P(None, "model")
    return jax.shard_map(
        functools.partial(on_lines if lines else plain, n_zero, n_model),
        mesh=mesh,
        in_specs=(tall, low, wide) * 3 + (P(("zero", "model")),) * 2,
        out_specs=(wide,) * 3 + (P("model"),) * 3 + (P(),),
        check_vma=False,
    )
```

```python
import functools

import jax
import jax.numpy as jnp
from jax import lax
from jax.experimental import pallas as pl
from jax.experimental.pallas import tpu as pltpu
from jax.sharding import PartitionSpec as P

MESH = pl.DeviceIdType.MESH
mix_rate = 0.5
VMEM_MOST = 67_043_328
SPARE = 65_536
COLUMNS = 2
SHARES = 32
PARTS = ((0, 0, 8), (0, 8, 8), (0, 16, 16), (1, 0, 15), (1, 15, 17), (2, 0, 8), (2, 8, 24))
PIECES = len(PARTS)
RAW = 2
LATE = (4, 5, 6)
LAST = 6
CORES = 2
LOW, NORM = PIECES, PIECES + 1
WRITES = 4
FIRST = 1


def last_of(z, core, length):
    end, inner = (0, 1) if z < length // 2 else (length - 1, length - 2)
    if core == 0:
        return (inner, 1) if z == end else None, (inner, 1) if z == inner else None
    return (length - 1 - end, 1) if z == end else None, (length - 1 - end, 0) if z == end else None


def queues_of(z, core, length):
    every = [LOW, *range(RAW + 1), NORM, *range(RAW + 1, PIECES)]
    late = list(LATE)
    early = [c for c in every if c not in late]
    out = {"up": [], "down": [], "side": []}
    if z < length - 1:
        out["up"] += [(z - s, 0, c) for s in range(z + 1) for c in every]
        if z == 0:
            out["up"] += [(0, 1, c) for c in every]
        if z == length - 2:
            out["up"] += [(z, 1, c) for c in late]
    if z > 0:
        out["down"] += [(z + s, 0, c) for s in range(length - z) for c in every]
        if z == length - 1:
            out["down"] += [(z, 1, c) for c in every]
        if z == 1:
            out["down"] += [(z, 1, c) for c in late]
    for b in sorted(range(length), key=lambda b: (abs(b - z), b)):
        pieces = every
        if (z, b) in ((0, 1), (length - 1, length - 2)):
            pieces = early
        if (z, b) in ((1, 0), (length - 2, length - 1)):
            pieces = []
        out["side"] += [(b, 0, c) for c in pieces]
    _, handed = last_of(z, core, length)
    if handed:
        name = "side" if core else "down" if z < length // 2 else "up"
        out[name].remove((*handed, LAST))
    return out


def order_of(core, length):
    size = [part[2] / 16 for part in PARTS] + [0.02, 0.01]
    queues = [queues_of(z, core, length) for z in range(length)]
    far = 1e9
    there = [{} for _ in range(length)]
    for z in range(length):
        for c in range(len(size)):
            there[z][z, 0, c] = 0.0
    for _ in range(4 * length):
        for z in range(length):
            for name, queue in queues[z].items():
                now = 0.0
                for b, o, c in queue:
                    now = max(now, there[z].get((b, o, c), far)) + size[c]
                    to = {"up": z + 1, "down": z - 1, "side": z}[name]
                    key = (b, 1 - o if name == "side" else o, c)
                    there[to][key] = now
    result = []
    for z in range(length):
        events = []
        for name, queue in queues[z].items():
            key = 0.0
            for at, (b, o, c) in enumerate(queue):
                key = max(key, there[z][b, o, c])
                events.append((key, at, name, b, o, c))
        assert max(e[0] for e in events) < far
        result.append((sorted(events), there[z]))
    return result


def gather_kernel(
    n_zero, n_model,
    w_q, w_k, w_v, l_q, l_k, l_v, h_q, h_k, h_v, n_a, n_b,
    s_q, s_k, s_v, factors, norms, hand,
    w_vm, h_vm, l_vm, lows, raws, sums, scales, n_vm,
    send_sem, recv_sem, load_sem, sum_sem, norm_sem, ready_sem,
):
    w, low, high = (w_q, w_k, w_v), (l_q, l_k, l_v), (h_q, h_k, h_v)
    served = (s_q, s_k, s_v)
    length = n_zero // COLUMNS
    zero, model = lax.axis_index("zero"), lax.axis_index("model")
    place, column = zero // COLUMNS, zero % COLUMNS
    rows, width = w_q.shape
    rank = l_q.shape[0]
    share = rows // SHARES
    raw_rows = raws.shape[0] // n_zero
    me = zero * n_model + model
    orders = [order_of(core, length) for core in range(CORES)]
    core_at = model % CORES

    barrier = pltpu.get_barrier_semaphore()
    partners = [(zero, lax.rem(model + k, n_model)) for k in range(1, n_model)]
    partners.append((place * COLUMNS + 1 - column, model))
    for to in partners:
        pl.semaphore_signal(barrier, inc=1, device_id=to, device_id_type=MESH)

    @pl.when(place > 0)
    def _():
        pl.semaphore_signal(barrier, inc=1, device_id=(zero - COLUMNS, model), device_id_type=MESH)

    @pl.when(place < length - 1)
    def _():
        pl.semaphore_signal(barrier, inc=1, device_id=(zero + COLUMNS, model), device_id_type=MESH)

    for i, (refs, into) in enumerate(((low, l_vm), (w, w_vm), (high, h_vm), ((n_a, n_b), n_vm))):
        for m, ref in enumerate(refs):
            pltpu.make_async_copy(ref, into.at[m], load_sem.at[i]).start()

    def block_at(b, o):
        return b * COLUMNS + (column if o == 0 else 1 - column)

    def landing(block, c):
        if c == LOW:
            return lows.at[block]
        if c == NORM:
            return norms.at[pl.ds(block * n_model, n_model)]
        m, first, many = PARTS[c]
        ref, tall = (raws, raw_rows) if c < RAW else (served[m], rows)
        first = pl.multiple_of(block * tall, share) + first * share
        return ref.at[pl.ds(pl.multiple_of(first, share), many * share)]

    def taken(ref, sem):
        pltpu.make_async_copy(ref, ref, sem).wait()

    def group_of(name, c):
        if c in (LOW, NORM):
            return 6 + c - LOW
        return PARTS[c][0] + 3 * (name == "side")

    def arrival(block, at, c):
        return recv_sem.at[lax.rem(block - at + n_zero - 1, n_zero), c]

    def copy_of(z, name, b, o, c):
        block = block_at(b, o)
        target = {
            "up": (z + 1) * COLUMNS + column,
            "down": (z - 1) * COLUMNS + column,
            "side": z * COLUMNS + 1 - column,
        }[name]
        source = landing(block, c)
        if b == z and o == 0:
            if c < RAW:
                m, first, many = PARTS[c]
                source = w[m].at[pl.ds(first * share, many * share)]
            if c == LOW:
                source = l_q.at[:, pl.ds(0, raw_rows)]
        return pltpu.make_async_remote_copy(
            src_ref=source,
            dst_ref=landing(block, c),
            send_sem=send_sem.at[group_of(name, c)],
            recv_sem=arrival(block, target, c),
            device_id=(target, model),
            device_id_type=MESH,
        )

    def arrive(b, o, c):
        block = block_at(b, o)
        taken(landing(block, c), arrival(block, zero, c))

    def send_own(z, pieces):
        for key, at, name, b, o, c in orders[0][z][0]:
            if b == z and o == 0 and c in pieces:
                copy_of(z, name, b, o, c).start()

    def send_all(pieces):
        for z in range(length):

            @pl.when(place == z)
            def _(z=z):
                send_own(z, pieces)

    def ready(z, way):
        pl.semaphore_signal(
            ready_sem.at[way], inc=1, device_id=(zero + (1 - 2 * way) * COLUMNS, model), device_id_type=MESH
        )

    for z in range(length):

        @pl.when(place == z)
        def _(z=z):
            pl.semaphore_wait(barrier, len(partners) + (z > 0) + (z < length - 1))
            send_own(z, (LOW, *range(FIRST)))
            for way in (0, 1):
                if (length - 1 - z, z)[way] and not (z, length - 1 - z)[way]:
                    ready(z, way)

    def relay(step):
        for z in range(length):
            way = step if z < length // 2 else 1 - step

            @pl.when(place == z)
            def _(z=z, way=way):
                if (z, length - 1 - z)[way]:
                    pl.semaphore_wait(ready_sem.at[way], 1)
                    if (length - 1 - z, z)[way]:
                        ready(z, way)

    for i, into in enumerate((l_vm, w_vm, h_vm, n_vm)):
        taken(into, load_sem.at[i])

    def whole_of(m, low_ref, source, at):
        mixed = lax.dot_general(
            low_ref[:, at], h_vm[m], (((0,), (0,)), ((), ())), preferred_element_type=jnp.float32
        )
        return source[at, :].astype(jnp.float32) + mix_rate * mixed

    tile = 128
    for m in range(3):

        def add(i, total, m=m):
            at = pl.ds(pl.multiple_of(i * tile, tile), tile)
            whole = whole_of(m, l_vm.at[m], w_vm.at[m], at)
            return total + jnp.sum(jnp.abs(whole).reshape(tile // 8, 8, width), axis=0)

        total = lax.fori_loop(0, rows // tile, add, jnp.zeros((8, width), jnp.float32))
        sums[zero, :, m * width : (m + 1) * width] = jnp.sum(total, axis=0, keepdims=True)
        if m < 2:
            relay(m)
    norms[pl.ds(me, 1)] = (n_vm[0] + n_vm[1])[None]

    def sum_copy(k):
        to = lax.rem(zero + k, n_zero)
        return pltpu.make_async_remote_copy(
            src_ref=sums.at[zero],
            dst_ref=sums.at[zero],
            send_sem=sum_sem.at[0],
            recv_sem=sum_sem.at[1],
            device_id=(to, model),
            device_id_type=MESH,
        )

    def norm_copy(k):
        return pltpu.make_async_remote_copy(
            src_ref=norms.at[me],
            dst_ref=norms.at[me],
            send_sem=norm_sem.at[0],
            recv_sem=norm_sem.at[1],
            device_id=partners[k - 1],
            device_id_type=MESH,
        )

    for k in range(1, n_zero):
        sum_copy(k).start()
    send_all(tuple(range(FIRST, RAW)))
    for k in range(1, n_model):
        norm_copy(k).start()

    taken(sums.at[pl.ds(0, n_zero - 1)], sum_sem.at[1])
    total = sums[0]
    for b in range(1, n_zero):
        total = total + sums[b]
    factor = total / (rows * n_zero)
    factors[...] = factor
    scales[...] = 1.0 / factor

    def finish(m, block, low_ref, source, start, many):
        base = pl.multiple_of(block * rows, rows)

        def step(i, carry):
            first = pl.multiple_of(start + i * tile, tile)
            whole = whole_of(m, low_ref, source, pl.ds(first, tile))
            to = pl.ds(pl.multiple_of(base + first, tile), tile)
            served[m][to, :] = (whole * scales[:, m * width : (m + 1) * width]).astype(s_q.dtype)
            return carry

        lax.fori_loop(0, many // tile, step, 0)

    def finish_own(m, start, many):
        finish(m, zero, l_vm.at[m], w_vm.at[m], start, many)

    finish_own(0, raw_rows, rows - raw_rows)
    finish_own(1, 0, rows)
    taken(norms.at[pl.ds(0, n_model - 1)], norm_sem.at[1])
    send_all((NORM, *(c for c in range(RAW, PIECES) if PARTS[c][0] == 0)))
    finish_own(2, 0, rows)
    send_all(tuple(c for c in range(RAW, PIECES) if PARTS[c][0] == 1))
    finish_own(0, 0, raw_rows)
    send_all(tuple(c for c in range(RAW, PIECES) if PARTS[c][0] == 2))
    def hand_on(b, o):
        block = block_at(b, o)
        m, first, many = PARTS[LAST]
        base = pl.multiple_of(block * rows, rows) + first * share

        def step(i, carry):
            at = pl.multiple_of(i * tile, tile)
            hand[pl.ds(at, tile), :] = served[m][pl.ds(pl.multiple_of(base + at, tile), tile), :]
            return carry

        lax.fori_loop(0, many * share // tile, step, 0)

    def serve(z, core):
        events, there = orders[core][z]
        lacking, handed = last_of(z, core, length)
        items = [(key, 0, at, name, b, o, c) for key, at, name, b, o, c in events]
        for b in range(length):
            for o in range(COLUMNS):
                if (b, o) != (z, 0):
                    when = max(there[b, o, c] for c in (*range(RAW), LOW))
                    items.append((when, 1, 0, "", b, o, 0))
        if handed:
            items.append((there[(*handed, LAST)], 2, 0, "", *handed, LAST))
        seen = {(z, 0, c) for c in range(PIECES + 2)}
        if lacking:
            seen.add((*lacking, LAST))

        def need(b, o, c):
            if (b, o, c) not in seen:
                seen.add((b, o, c))
                arrive(b, o, c)

        for _, kind, _, name, b, o, c in sorted(items):
            if kind == 0:
                if (b, o) != (z, 0):
                    need(b, o, c)
                    copy_of(z, name, b, o, c).start()
            elif kind == 1:
                for piece in (*range(RAW), LOW):
                    need(b, o, piece)
                block = block_at(b, o)
                raw = raws.at[pl.ds(pl.multiple_of(block * raw_rows, raw_rows), raw_rows)]
                finish(0, block, lows.at[block], raw, 0, raw_rows)
            else:
                need(b, o, c)
                hand_on(b, o)
        for b in range(length):
            for o in range(COLUMNS):
                for c in range(PIECES + 2):
                    need(b, o, c)
        sent = [0] * 8
        for key, at, name, b, o, c in events:
            sent[group_of(name, c)] += 1 if c in (LOW, NORM) else PARTS[c][2] * share
        sent[7] *= n_model
        for i, many in enumerate(sent):
            if many:
                taken((lows, norms)[i - 6].at[pl.ds(0, many)] if i > 5 else s_q.at[pl.ds(0, many)], send_sem.at[i])

    for z in range(length):
        for core in range(CORES):
            pl.when((place == z) & (core_at == core))(functools.partial(serve, z, core))

    taken(sums.at[pl.ds(0, n_zero - 1)], sum_sem.at[0])
    taken(norms.at[pl.ds(0, n_model - 1)], norm_sem.at[0])


def write_kernel(s_q, s_k, s_v, factors, norms, o_q, o_k, o_v, f_q, f_k, f_v, norm, norm_vm, sem):
    rows = s_q.shape[0] // WRITES
    width = s_q.shape[1]
    copies = []
    for m, (s, o) in enumerate(((s_q, o_q), (s_k, o_k), (s_v, o_v))):
        for i in range(WRITES):
            part = pl.ds(i * rows, rows)
            copies.append((s.at[part], o.at[part]))
    for m, f in enumerate((f_q, f_k, f_v)):
        copies.append((factors.at[:, pl.ds(m * width, width)], f))
    copies.append((norm_vm, norm))
    copies = [pltpu.make_async_copy(s, o, sem.at[i]) for i, (s, o) in enumerate(copies)]
    for copy in copies[:-1]:
        copy.start()
    norm_vm[...] = norms[...].reshape(norm.shape).astype(norm.dtype)
    copies[-1].start()
    for copy in copies:
        copy.wait()


def last_kernel(n_zero, n_model, given, late, out, sem):
    length = n_zero // COLUMNS
    zero, model = lax.axis_index("zero"), lax.axis_index("model")
    place, column, core_at = zero // COLUMNS, zero % COLUMNS, model % CORES
    rows = out.shape[0] // n_zero
    first = PARTS[LAST][1] * (rows // SHARES)
    for z in (0, length - 1):
        for core in range(CORES):
            lacking, _ = last_of(z, core, length)

            @pl.when((place == z) & (core_at == core))
            def _(b=lacking[0]):
                block = b * COLUMNS + 1 - column
                base = pl.multiple_of(block * rows, rows) + first
                part = out.at[pl.ds(pl.multiple_of(base, rows // SHARES), late.shape[0])]
                copy = pltpu.make_async_copy(late, part, sem)
                copy.start()
                copy.wait()


def on_lines(n_zero, n_model, w_q, l_q, h_q, w_k, l_k, h_k, w_v, l_v, h_v, n_a, n_b):
    rows, width = w_q.shape
    rank = l_q.shape[1]
    d_model = rows * n_zero
    count = n_zero * n_model
    share = n_a.shape[0]
    raw_rows = sum(part[2] for part in PARTS[:RAW]) * rows // SHARES
    f32, bf16 = jnp.float32, jnp.bfloat16
    shape = jax.ShapeDtypeStruct
    anywhere = pl.BlockSpec(memory_space=pl.ANY)
    inside = pl.BlockSpec(memory_space=pltpu.VMEM)
    dma = pltpu.SemaphoreType.DMA
    tall = (d_model, width)
    hand_rows = PARTS[LAST][2] * rows // SHARES
    s_q, s_k, s_v, factors, norms, hand = pl.pallas_call(
        functools.partial(gather_kernel, n_zero, n_model),
        out_shape=(pltpu.VMEM(tall, bf16),) * 3
        + (pltpu.VMEM((1, 3 * width), f32), pltpu.VMEM((count, 1, share), f32), pltpu.VMEM((hand_rows, width), bf16)),
        in_specs=[anywhere] * 11,
        out_specs=(inside,) * 6,
        scratch_shapes=[
            pltpu.VMEM((3, rows, width), bf16),
            pltpu.VMEM((3, rank, width), bf16),
            pltpu.VMEM((3, rank, rows), bf16),
            pltpu.VMEM((n_zero, rank, raw_rows), bf16),
            pltpu.VMEM((n_zero * raw_rows, width), bf16),
            pltpu.VMEM((n_zero, 1, 3 * width), f32),
            pltpu.VMEM((1, 3 * width), f32),
            pltpu.VMEM((2, 1, share), f32),
            dma((8,)),
            dma((n_zero - 1, PIECES + 2)),
            dma((4,)),
            dma((2,)),
            dma((2,)),
            pltpu.SemaphoreType.REGULAR((2,)),
        ],
        compiler_params=pltpu.CompilerParams(
            collective_id=0, has_side_effects=True, vmem_limit_bytes=VMEM_MOST - 3 * d_model * width * 2 - 8 * hand_rows * width - SPARE
        ),
    )(w_q, w_k, w_v, l_q.T, l_k.T, l_v.T, h_q, h_k, h_v, n_a.reshape(1, share), n_b.reshape(1, share))
    pairs = []
    for zero in range(n_zero):
        for model in range(n_model):
            z, column, core = zero // COLUMNS, zero % COLUMNS, model % CORES
            lacking, _ = last_of(z, core, n_zero // COLUMNS)
            if lacking:
                giver = (z * COLUMNS + 1 - column) if core else lacking[0] * COLUMNS + column
                pairs.append((giver * n_model + model, zero * n_model + model))
    late = lax.ppermute(hand, ("zero", "model"), pairs)
    *served, f_q, f_k, f_v, norm = pl.pallas_call(
        write_kernel,
        out_shape=(shape(tall, bf16),) * 3 + (shape((1, width), f32),) * 3 + (shape((count, share), bf16),),
        in_specs=[anywhere] * 3 + [inside] * 2,
        out_specs=(anywhere,) * 7,
        scratch_shapes=[pltpu.VMEM((count, share), bf16), dma((3 * WRITES + 4,))],
        compiler_params=pltpu.CompilerParams(
            vmem_limit_bytes=4 * 1024 * 1024
        ),
        cost_estimate=pl.CostEstimate(flops=10**9, bytes_accessed=12 * d_model * width, transcendentals=0),
    )(s_q, s_k, s_v, factors, norms)
    served[2] = pl.pallas_call(
        functools.partial(last_kernel, n_zero, n_model),
        out_shape=shape(tall, bf16),
        in_specs=[anywhere] * 2,
        out_specs=anywhere,
        scratch_shapes=[dma],
        input_output_aliases={0: 0},
        compiler_params=pltpu.CompilerParams(vmem_limit_bytes=1024 * 1024),
    )(served[2], late)
    return (*served, f_q.reshape(width), f_k.reshape(width), f_v.reshape(width), norm.reshape(count * share))


def plain(n_zero, n_model, w_q, l_q, h_q, w_k, l_k, h_k, w_v, l_v, h_v, n_a, n_b):
    d_model = w_q.shape[0] * n_zero
    wholes = [
        w.astype(jnp.float32) + mix_rate * jnp.dot(l, h, preferred_element_type=jnp.float32)
        for w, l, h in ((w_q, l_q, h_q), (w_k, l_k, h_k), (w_v, l_v, h_v))
    ]
    totals = lax.psum([jnp.sum(jnp.abs(whole), axis=0) for whole in wholes], "zero")
    factors = [total / d_model for total in totals]
    serving = [
        lax.all_gather((whole / factor).astype(jnp.bfloat16), "zero", axis=0, tiled=True)
        for whole, factor in zip(wholes, factors)
    ]
    norm = lax.all_gather(
        (n_a + n_b).astype(jnp.bfloat16), ("zero", "model"), axis=0, tiled=True
    )
    return (*serving, *factors, norm)


def solution(mesh):
    n_zero, n_model = mesh.shape["zero"], mesh.shape["model"]
    lines = n_zero == 2 * n_model
    tall, low, wide = P("zero", "model"), P("zero", None), P(None, "model")
    return jax.shard_map(
        functools.partial(on_lines if lines else plain, n_zero, n_model),
        mesh=mesh,
        in_specs=(tall, low, wide) * 3 + (P(("zero", "model")),) * 2,
        out_specs=(wide,) * 3 + (P("model"),) * 3 + (P(),),
        check_vma=False,
    )
```

```python
import functools

import jax
import jax.numpy as jnp
from jax import lax
from jax.experimental import pallas as pl
from jax.experimental.pallas import tpu as pltpu
from jax.sharding import PartitionSpec as P

MESH = pl.DeviceIdType.MESH
mix_rate = 0.5
VMEM_MOST = 67_043_328
SPARE = 65_536
COLUMNS = 2
SHARES = 32
PARTS = ((0, 0, 8), (0, 8, 8), (0, 16, 16), (1, 0, 15), (1, 15, 17), (2, 0, 8), (2, 8, 24))
PIECES = len(PARTS)
RAW = 2
LATE = (4, 5, 6)
LAST = 6
CORES = 2
LOW, NORM = PIECES, PIECES + 1
WRITES = 4
FIRST = 1


def last_of(z, core, length):
    end, inner = (0, 1) if z < length // 2 else (length - 1, length - 2)
    if core == 0:
        return (inner, 1) if z == end else None, (inner, 1) if z == inner else None
    return (length - 1 - end, 1) if z == end else None, (length - 1 - end, 0) if z == end else None


def queues_of(z, core, length):
    every = [LOW, *range(RAW + 1), NORM, *range(RAW + 1, PIECES)]
    late = list(LATE)
    early = [c for c in every if c not in late]
    out = {"up": [], "down": [], "side": []}
    if z < length - 1:
        out["up"] += [(z - s, 0, c) for s in range(z + 1) for c in every]
        if z == 0:
            out["up"] += [(0, 1, c) for c in every]
        if z == length - 2:
            out["up"] += [(z, 1, c) for c in late]
    if z > 0:
        out["down"] += [(z + s, 0, c) for s in range(length - z) for c in every]
        if z == length - 1:
            out["down"] += [(z, 1, c) for c in every]
        if z == 1:
            out["down"] += [(z, 1, c) for c in late]
    for b in sorted(range(length), key=lambda b: (abs(b - z), b)):
        pieces = every
        if (z, b) in ((0, 1), (length - 1, length - 2)):
            pieces = early
        if (z, b) in ((1, 0), (length - 2, length - 1)):
            pieces = []
        out["side"] += [(b, 0, c) for c in pieces]
    _, handed = last_of(z, core, length)
    if handed:
        name = "side" if core else "down" if z < length // 2 else "up"
        out[name].remove((*handed, LAST))
    return out


def order_of(core, length):
    size = [part[2] / 16 for part in PARTS] + [0.02, 0.01]
    queues = [queues_of(z, core, length) for z in range(length)]
    far = 1e9
    there = [{} for _ in range(length)]
    for z in range(length):
        for c in range(len(size)):
            there[z][z, 0, c] = 0.0
    for _ in range(4 * length):
        for z in range(length):
            for name, queue in queues[z].items():
                now = 0.0
                for b, o, c in queue:
                    now = max(now, there[z].get((b, o, c), far)) + size[c]
                    to = {"up": z + 1, "down": z - 1, "side": z}[name]
                    key = (b, 1 - o if name == "side" else o, c)
                    there[to][key] = now
    result = []
    for z in range(length):
        events = []
        for name, queue in queues[z].items():
            key = 0.0
            for at, (b, o, c) in enumerate(queue):
                key = max(key, there[z][b, o, c])
                events.append((key, at, name, b, o, c))
        assert max(e[0] for e in events) < far
        result.append((sorted(events), there[z]))
    return result


def gather_kernel(
    n_zero, n_model,
    w_q, w_k, w_v, l_q, l_k, l_v, h_q, h_k, h_v, n_a, n_b,
    s_q, s_k, s_v, factors, norms, hand,
    w_vm, h_vm, l_vm, lows, raws, sums, scales, n_vm,
    send_sem, recv_sem, load_sem, sum_sem, norm_sem, ready_sem,
):
    w, low, high = (w_q, w_k, w_v), (l_q, l_k, l_v), (h_q, h_k, h_v)
    served = (s_q, s_k, s_v)
    length = n_zero // COLUMNS
    zero, model = lax.axis_index("zero"), lax.axis_index("model")
    place, column = zero // COLUMNS, zero % COLUMNS
    rows, width = w_q.shape
    rank = l_q.shape[0]
    share = rows // SHARES
    raw_rows = raws.shape[0] // n_zero
    me = zero * n_model + model
    orders = [order_of(core, length) for core in range(CORES)]
    core_at = model % CORES

    barrier = pltpu.get_barrier_semaphore()
    partners = [(zero, lax.rem(model + k, n_model)) for k in range(1, n_model)]
    partners.append((place * COLUMNS + 1 - column, model))
    for to in partners:
        pl.semaphore_signal(barrier, inc=1, device_id=to, device_id_type=MESH)

    @pl.when(place > 0)
    def _():
        pl.semaphore_signal(barrier, inc=1, device_id=(zero - COLUMNS, model), device_id_type=MESH)

    @pl.when(place < length - 1)
    def _():
        pl.semaphore_signal(barrier, inc=1, device_id=(zero + COLUMNS, model), device_id_type=MESH)

    for i, (refs, into) in enumerate(((low, l_vm), (w, w_vm), (high, h_vm), ((n_a, n_b), n_vm))):
        for m, ref in enumerate(refs):
            pltpu.make_async_copy(ref, into.at[m], load_sem.at[i]).start()

    def block_at(b, o):
        return b * COLUMNS + (column if o == 0 else 1 - column)

    def landing(block, c):
        if c == LOW:
            return lows.at[block]
        if c == NORM:
            return norms.at[pl.ds(block * n_model, n_model)]
        m, first, many = PARTS[c]
        ref, tall = (raws, raw_rows) if c < RAW else (served[m], rows)
        first = pl.multiple_of(block * tall, share) + first * share
        return ref.at[pl.ds(pl.multiple_of(first, share), many * share)]

    def taken(ref, sem):
        pltpu.make_async_copy(ref, ref, sem).wait()

    def group_of(name, c):
        if c in (LOW, NORM):
            return 6 + c - LOW
        return PARTS[c][0] + 3 * (name == "side")

    def arrival(block, at, c):
        return recv_sem.at[lax.rem(block - at + n_zero - 1, n_zero), max(c - RAW + 1, 0)]

    def copy_of(z, name, b, o, c):
        block = block_at(b, o)
        target = {
            "up": (z + 1) * COLUMNS + column,
            "down": (z - 1) * COLUMNS + column,
            "side": z * COLUMNS + 1 - column,
        }[name]
        source = landing(block, c)
        if b == z and o == 0:
            if c < RAW:
                m, first, many = PARTS[c]
                source = w[m].at[pl.ds(first * share, many * share)]
            if c == LOW:
                source = l_q.at[:, pl.ds(0, raw_rows)]
        return pltpu.make_async_remote_copy(
            src_ref=source,
            dst_ref=landing(block, c),
            send_sem=send_sem.at[group_of(name, c)],
            recv_sem=arrival(block, target, c),
            device_id=(target, model),
            device_id_type=MESH,
        )

    def arrive(b, o, c):
        block = block_at(b, o)
        raw = raws.at[pl.ds(pl.multiple_of(block * raw_rows, raw_rows), raw_rows)]
        taken(raw if c < RAW else landing(block, c), arrival(block, zero, c))

    def send_own(z, pieces):
        for key, at, name, b, o, c in orders[0][z][0]:
            if b == z and o == 0 and c in pieces:
                copy_of(z, name, b, o, c).start()

    def send_all(pieces):
        for z in range(length):

            @pl.when(place == z)
            def _(z=z):
                send_own(z, pieces)

    def ready(z, way):
        pl.semaphore_signal(
            ready_sem.at[way], inc=1, device_id=(zero + (1 - 2 * way) * COLUMNS, model), device_id_type=MESH
        )

    for z in range(length):

        @pl.when(place == z)
        def _(z=z):
            pl.semaphore_wait(barrier, len(partners) + (z > 0) + (z < length - 1))
            send_own(z, (LOW, *range(FIRST)))
            for way in (0, 1):
                if (length - 1 - z, z)[way] and not (z, length - 1 - z)[way]:
                    ready(z, way)

    def relay(step):
        for z in range(length):
            way = step if z < length // 2 else 1 - step

            @pl.when(place == z)
            def _(z=z, way=way):
                if (z, length - 1 - z)[way]:
                    pl.semaphore_wait(ready_sem.at[way], 1)
                    if (length - 1 - z, z)[way]:
                        ready(z, way)

    for i, into in enumerate((l_vm, w_vm, h_vm, n_vm)):
        taken(into, load_sem.at[i])

    def whole_of(m, low_ref, source, at):
        mixed = lax.dot_general(
            low_ref[:, at], h_vm[m], (((0,), (0,)), ((), ())), preferred_element_type=jnp.float32
        )
        return source[at, :].astype(jnp.float32) + mix_rate * mixed

    tile = 128
    for m in range(3):

        def add(i, total, m=m):
            at = pl.ds(pl.multiple_of(i * tile, tile), tile)
            whole = whole_of(m, l_vm.at[m], w_vm.at[m], at)
            return total + jnp.sum(jnp.abs(whole).reshape(tile // 8, 8, width), axis=0)

        total = lax.fori_loop(0, rows // tile, add, jnp.zeros((8, width), jnp.float32))
        sums[zero, :, m * width : (m + 1) * width] = jnp.sum(total, axis=0, keepdims=True)
        if m < 2:
            relay(m)
    norms[pl.ds(me, 1)] = (n_vm[0] + n_vm[1])[None]

    def sum_copy(k):
        to = lax.rem(zero + k, n_zero)
        return pltpu.make_async_remote_copy(
            src_ref=sums.at[zero],
            dst_ref=sums.at[zero],
            send_sem=sum_sem.at[0],
            recv_sem=sum_sem.at[1],
            device_id=(to, model),
            device_id_type=MESH,
        )

    def norm_copy(k):
        return pltpu.make_async_remote_copy(
            src_ref=norms.at[me],
            dst_ref=norms.at[me],
            send_sem=norm_sem.at[0],
            recv_sem=norm_sem.at[1],
            device_id=partners[k - 1],
            device_id_type=MESH,
        )

    for k in range(1, n_zero):
        sum_copy(k).start()
    send_all(tuple(range(FIRST, RAW)))
    for k in range(1, n_model):
        norm_copy(k).start()

    taken(sums.at[pl.ds(0, n_zero - 1)], sum_sem.at[1])
    total = sums[0]
    for b in range(1, n_zero):
        total = total + sums[b]
    factor = total / (rows * n_zero)
    factors[...] = factor
    scales[...] = 1.0 / factor

    def finish(m, block, low_ref, source, start, many):
        base = pl.multiple_of(block * rows, rows)

        def step(i, carry):
            first = pl.multiple_of(start + i * tile, tile)
            whole = whole_of(m, low_ref, source, pl.ds(first, tile))
            to = pl.ds(pl.multiple_of(base + first, tile), tile)
            served[m][to, :] = (whole * scales[:, m * width : (m + 1) * width]).astype(s_q.dtype)
            return carry

        lax.fori_loop(0, many // tile, step, 0)

    def finish_own(m, start, many):
        finish(m, zero, l_vm.at[m], w_vm.at[m], start, many)

    finish_own(0, raw_rows, rows - raw_rows)
    finish_own(1, 0, rows // 2)
    taken(norms.at[pl.ds(0, n_model - 1)], norm_sem.at[1])
    send_all((NORM, *(c for c in range(RAW, PIECES) if PARTS[c][0] == 0)))
    finish_own(1, rows // 2, rows // 2)
    finish_own(2, 0, rows)
    send_all(tuple(c for c in range(RAW, PIECES) if PARTS[c][0] == 1))
    finish_own(0, 0, raw_rows)
    send_all(tuple(c for c in range(RAW, PIECES) if PARTS[c][0] == 2))
    def hand_on(b, o):
        block = block_at(b, o)
        m, first, many = PARTS[LAST]
        base = pl.multiple_of(block * rows, rows) + first * share

        def step(i, carry):
            at = pl.multiple_of(i * tile, tile)
            hand[pl.ds(at, tile), :] = served[m][pl.ds(pl.multiple_of(base + at, tile), tile), :]
            return carry

        lax.fori_loop(0, many * share // tile, step, 0)

    def serve(z, core):
        events, there = orders[core][z]
        lacking, handed = last_of(z, core, length)
        items = [(key, 0, at, name, b, o, c) for key, at, name, b, o, c in events]
        for b in range(length):
            for o in range(COLUMNS):
                if (b, o) != (z, 0):
                    when = max(there[b, o, c] for c in (*range(RAW), LOW))
                    items.append((when, 1, 0, "", b, o, 0))
        if handed:
            items.append((there[(*handed, LAST)], 2, 0, "", *handed, LAST))
        seen = {(z, 0, c) for c in range(PIECES + 2)}
        if lacking:
            seen.add((*lacking, LAST))

        def need(b, o, c):
            if (b, o, c) not in seen:
                seen.update((b, o, piece) for piece in (range(RAW) if c < RAW else (c,)))
                arrive(b, o, c)

        for _, kind, _, name, b, o, c in sorted(items):
            if kind == 0:
                if (b, o) != (z, 0):
                    need(b, o, c)
                    copy_of(z, name, b, o, c).start()
            elif kind == 1:
                for piece in (*range(RAW), LOW):
                    need(b, o, piece)
                block = block_at(b, o)
                raw = raws.at[pl.ds(pl.multiple_of(block * raw_rows, raw_rows), raw_rows)]
                finish(0, block, lows.at[block], raw, 0, raw_rows)
            else:
                need(b, o, c)
                hand_on(b, o)
        for b in range(length):
            for o in range(COLUMNS):
                for c in range(PIECES + 2):
                    need(b, o, c)
        sent = [0] * 8
        for key, at, name, b, o, c in events:
            sent[group_of(name, c)] += 1 if c in (LOW, NORM) else PARTS[c][2] * share
        sent[7] *= n_model
        for i, many in enumerate(sent):
            if many:
                taken((lows, norms)[i - 6].at[pl.ds(0, many)] if i > 5 else s_q.at[pl.ds(0, many)], send_sem.at[i])

    for z in range(length):
        for core in range(CORES):
            pl.when((place == z) & (core_at == core))(functools.partial(serve, z, core))

    taken(sums.at[pl.ds(0, n_zero - 1)], sum_sem.at[0])
    taken(norms.at[pl.ds(0, n_model - 1)], norm_sem.at[0])


def write_kernel(s_q, s_k, s_v, factors, norms, o_q, o_k, o_v, f_q, f_k, f_v, norm, norm_vm, sem):
    rows = s_q.shape[0] // WRITES
    width = s_q.shape[1]
    copies = []
    for m, (s, o) in enumerate(((s_q, o_q), (s_k, o_k), (s_v, o_v))):
        for i in range(WRITES):
            part = pl.ds(i * rows, rows)
            copies.append((s.at[part], o.at[part]))
    for m, f in enumerate((f_q, f_k, f_v)):
        copies.append((factors.at[:, pl.ds(m * width, width)], f))
    copies.append((norm_vm, norm))
    copies = [pltpu.make_async_copy(s, o, sem.at[i]) for i, (s, o) in enumerate(copies)]
    for copy in copies[:-1]:
        copy.start()
    norm_vm[...] = norms[...].reshape(norm.shape).astype(norm.dtype)
    copies[-1].start()
    for copy in copies:
        copy.wait()


def last_kernel(n_zero, n_model, given, late, out, sem):
    length = n_zero // COLUMNS
    zero, model = lax.axis_index("zero"), lax.axis_index("model")
    place, column, core_at = zero // COLUMNS, zero % COLUMNS, model % CORES
    rows = out.shape[0] // n_zero
    first = PARTS[LAST][1] * (rows // SHARES)
    for z in (0, length - 1):
        for core in range(CORES):
            lacking, _ = last_of(z, core, length)

            @pl.when((place == z) & (core_at == core))
            def _(b=lacking[0]):
                block = b * COLUMNS + 1 - column
                base = pl.multiple_of(block * rows, rows) + first
                part = out.at[pl.ds(pl.multiple_of(base, rows // SHARES), late.shape[0])]
                copy = pltpu.make_async_copy(late, part, sem)
                copy.start()
                copy.wait()


def on_lines(n_zero, n_model, w_q, l_q, h_q, w_k, l_k, h_k, w_v, l_v, h_v, n_a, n_b):
    rows, width = w_q.shape
    rank = l_q.shape[1]
    d_model = rows * n_zero
    count = n_zero * n_model
    share = n_a.shape[0]
    raw_rows = sum(part[2] for part in PARTS[:RAW]) * rows // SHARES
    f32, bf16 = jnp.float32, jnp.bfloat16
    shape = jax.ShapeDtypeStruct
    anywhere = pl.BlockSpec(memory_space=pl.ANY)
    inside = pl.BlockSpec(memory_space=pltpu.VMEM)
    dma = pltpu.SemaphoreType.DMA
    tall = (d_model, width)
    hand_rows = PARTS[LAST][2] * rows // SHARES
    s_q, s_k, s_v, factors, norms, hand = pl.pallas_call(
        functools.partial(gather_kernel, n_zero, n_model),
        out_shape=(pltpu.VMEM(tall, bf16),) * 3
        + (pltpu.VMEM((1, 3 * width), f32), pltpu.VMEM((count, 1, share), f32), pltpu.VMEM((hand_rows, width), bf16)),
        in_specs=[anywhere] * 11,
        out_specs=(inside,) * 6,
        scratch_shapes=[
            pltpu.VMEM((3, rows, width), bf16),
            pltpu.VMEM((3, rank, width), bf16),
            pltpu.VMEM((3, rank, rows), bf16),
            pltpu.VMEM((n_zero, rank, raw_rows), bf16),
            pltpu.VMEM((n_zero * raw_rows, width), bf16),
            pltpu.VMEM((n_zero, 1, 3 * width), f32),
            pltpu.VMEM((1, 3 * width), f32),
            pltpu.VMEM((2, 1, share), f32),
            dma((8,)),
            dma((n_zero - 1, PIECES + 3 - RAW)),
            dma((4,)),
            dma((2,)),
            dma((2,)),
            pltpu.SemaphoreType.REGULAR((2,)),
        ],
        compiler_params=pltpu.CompilerParams(
            collective_id=0, has_side_effects=True, vmem_limit_bytes=VMEM_MOST - 3 * d_model * width * 2 - 8 * hand_rows * width - SPARE
        ),
    )(w_q, w_k, w_v, l_q.T, l_k.T, l_v.T, h_q, h_k, h_v, n_a.reshape(1, share), n_b.reshape(1, share))
    pairs = []
    for zero in range(n_zero):
        for model in range(n_model):
            z, column, core = zero // COLUMNS, zero % COLUMNS, model % CORES
            lacking, _ = last_of(z, core, n_zero // COLUMNS)
            if lacking:
                giver = (z * COLUMNS + 1 - column) if core else lacking[0] * COLUMNS + column
                pairs.append((giver * n_model + model, zero * n_model + model))
    late = lax.ppermute(hand, ("zero", "model"), pairs)
    *served, f_q, f_k, f_v, norm = pl.pallas_call(
        write_kernel,
        out_shape=(shape(tall, bf16),) * 3 + (shape((1, width), f32),) * 3 + (shape((count, share), bf16),),
        in_specs=[anywhere] * 3 + [inside] * 2,
        out_specs=(anywhere,) * 7,
        scratch_shapes=[pltpu.VMEM((count, share), bf16), dma((3 * WRITES + 4,))],
        compiler_params=pltpu.CompilerParams(
            vmem_limit_bytes=4 * 1024 * 1024
        ),
        cost_estimate=pl.CostEstimate(flops=10**9, bytes_accessed=12 * d_model * width, transcendentals=0),
    )(s_q, s_k, s_v, factors, norms)
    served[2] = pl.pallas_call(
        functools.partial(last_kernel, n_zero, n_model),
        out_shape=shape(tall, bf16),
        in_specs=[anywhere] * 2,
        out_specs=anywhere,
        scratch_shapes=[dma],
        input_output_aliases={0: 0},
        compiler_params=pltpu.CompilerParams(vmem_limit_bytes=1024 * 1024),
    )(served[2], late)
    return (*served, f_q.reshape(width), f_k.reshape(width), f_v.reshape(width), norm.reshape(count * share))


def plain(n_zero, n_model, w_q, l_q, h_q, w_k, l_k, h_k, w_v, l_v, h_v, n_a, n_b):
    d_model = w_q.shape[0] * n_zero
    wholes = [
        w.astype(jnp.float32) + mix_rate * jnp.dot(l, h, preferred_element_type=jnp.float32)
        for w, l, h in ((w_q, l_q, h_q), (w_k, l_k, h_k), (w_v, l_v, h_v))
    ]
    totals = lax.psum([jnp.sum(jnp.abs(whole), axis=0) for whole in wholes], "zero")
    factors = [total / d_model for total in totals]
    serving = [
        lax.all_gather((whole / factor).astype(jnp.bfloat16), "zero", axis=0, tiled=True)
        for whole, factor in zip(wholes, factors)
    ]
    norm = lax.all_gather(
        (n_a + n_b).astype(jnp.bfloat16), ("zero", "model"), axis=0, tiled=True
    )
    return (*serving, *factors, norm)


def solution(mesh):
    n_zero, n_model = mesh.shape["zero"], mesh.shape["model"]
    lines = n_zero == 2 * n_model
    tall, low, wide = P("zero", "model"), P("zero", None), P(None, "model")
    return jax.shard_map(
        functools.partial(on_lines if lines else plain, n_zero, n_model),
        mesh=mesh,
        in_specs=(tall, low, wide) * 3 + (P(("zero", "model")),) * 2,
        out_specs=(wide,) * 3 + (P("model"),) * 3 + (P(),),
        check_vma=False,
    )
```
